32 devices in a mesh: sub: 8 (over z, y), inner: 4 (over x, core).
Axes of the slice: x: 2, y: 2, z: 4, core: 2. Of those that a mesh axis runs over, the one named last changes fastest.
Arguments:
- solution: float32 [32, 3, 32, 16, 128], P(None, None, 'sub', 'inner'), may hold values from -6 to 6
- residual: float32 [32, 3, 32, 16, 128], P(None, None, 'sub', 'inner'), may hold values from -6 to 6
- direction: float32 [32, 3, 32, 16, 128], P(None, None, 'sub', 'inner'), may hold values from -6 to 6
- mass: float32 [32, 16, 128], P('sub', 'inner'), may hold values from 0.2 to 5
- coarse_basis: float32 [32, 3, 32, 16, 128], P(None, None, 'sub', 'inner'), may hold values from -1 to 1
- line_inverse: float32 [8, 4, 128, 128], P('sub', 'inner'), may hold values from -1.5 to 1.5
- coarse_factor: float32 [1024, 1024], P(('sub', 'inner')), may hold values from -1 to 1
Outputs:
- new_solution: float32 [32, 3, 32, 16, 128], P(None, None, 'sub', 'inner')
- new_residual: float32 [32, 3, 32, 16, 128], P(None, None, 'sub', 'inner')
- new_direction: float32 [32, 3, 32, 16, 128], P(None, None, 'sub', 'inner')
The draws below stay inside these ranges and needn't reach their ends.
All inputs are finite; a program needn't handle non-finite values.
Results may differ from the reference program's by a relative error of at most 0.00017.
Values sent between devices are 32-bit elements; how exact they have to be, the bound alone decides.
A program may use at most 64 MiB of HBM per device.

```python
import math
import jax
import jax.numpy as jnp
from jax import lax

K = 32
NB = 32
CX = 4
CY = 4
CZ = 128
NX = 32
NY = 16
NZ = 128
NCOARSE = 1024
N_SUB = 8
N_INNER = 4


def paired_fields(key):
    first = jax.random.fold_in(key, 31)
    second = jax.random.fold_in(key, 32)
    shape = (K, 3, NX, NY, NZ)
    base = jnp.clip(jax.random.normal(first, shape, jnp.float32), -6.0, 6.0)
    noise = jnp.clip(jax.random.normal(second, shape, jnp.float32), -4.0, 4.0)
    moved = jnp.clip(base + 0.3 * noise, -6.0, 6.0)
    return (base, moved)


def draw_residual(key, part):
    return paired_fields(key)[0]


def draw_direction(key, part):
    return paired_fields(key)[1]


def draw_coarse_basis(key, part):
    return jax.random.uniform(key, (NB, 3, NX, NY, NZ), jnp.float32, -1.0, 1.0)


def draw_line_inverse(key, part):
    first = jax.random.fold_in(key, 11)
    second = jax.random.fold_in(key, 12)
    diagonal = jax.random.uniform(first, (N_SUB, N_INNER, CZ), jnp.float32, 0.5, 1.5)
    noise = jnp.clip(jax.random.normal(second, (N_SUB, N_INNER, CZ, CZ), jnp.float32), -4.0, 4.0)
    symmetric = (noise + jnp.swapaxes(noise, 2, 3)) * (0.35 / CZ ** 0.5)
    eye = jnp.eye(CZ, dtype=jnp.float32)
    return symmetric * (1.0 - eye) + diagonal[..., None] * eye


def draw_coarse_factor(key, part):
    first = jax.random.fold_in(key, 21)
    second = jax.random.fold_in(key, 22)
    factor = 0.7 * (3.0 * CX * CY * CZ * NB) ** (-0.25)
    diagonal = jax.random.uniform(first, (NCOARSE,), jnp.float32, 0.5, 1.5)
    noise = jnp.clip(jax.random.normal(second, (NCOARSE, NCOARSE), jnp.float32), -4.0, 4.0)
    eye = jnp.eye(NCOARSE, dtype=jnp.float32)
    matrix = noise * (0.5 / NCOARSE ** 0.5) * (1.0 - eye) + diagonal[:, None] * eye
    return matrix * factor


def levels(own_key, dims, cuts, smallest, high):
    gain = 1.0
    for dim, parts in cuts:
        heights = jax.random.uniform(jax.random.fold_in(jax.random.fold_in(own_key, 6), dim), (parts,), jnp.float32, smallest / len(cuts), high / len(cuts))
        gain = gain * jnp.repeat(jnp.exp(heights), dims[dim] // parts).reshape((-1,) + (1,) * (len(dims) - 1 - dim))
    return gain


def scatter_about(stream_key, shape, deviation, most, split=(), held_as=jnp.bfloat16):
    entries = jax.random.normal(stream_key, shape, jnp.float32) * deviation
    if len(split) > 0:
        entries = levels(stream_key, shape, split, -0.22, 0.18) * entries
    return jnp.clip(entries, min=-most, max=most).astype(held_as)


def setup_inputs(seed: int = 0) -> dict:
    key_of = jax.random.split(jax.random.key(seed), 8)
    solution = scatter_about(key_of[0], (K, 3, NX, NY, NZ), 1.0, 6.0, ((2, 8), (3, 4)), jnp.float32)
    residual = draw_residual(jax.random.fold_in(key_of[7], 71), 0)
    direction = draw_direction(jax.random.fold_in(key_of[7], 71), 0)
    mass = jnp.clip(jnp.exp(math.log(5.0) - 3.218876 * jax.random.uniform(key_of[3], (NX, NY, NZ), jnp.float32) ** levels(key_of[3], (NX, NY, NZ), ((0, 8), (1, 4)), -0.2, 0.2)), 0.2, 5.0)
    coarse_basis = draw_coarse_basis(jax.random.fold_in(key_of[7], 71), 0)
    line_inverse = draw_line_inverse(jax.random.fold_in(key_of[7], 71), 0)
    coarse_factor = draw_coarse_factor(jax.random.fold_in(key_of[7], 71), 0)
    return {"solution": solution, "residual": residual, "direction": direction, "mass": mass, "coarse_basis": coarse_basis, "line_inverse": line_inverse, "coarse_factor": coarse_factor}


exact_mode = lax.Precision.HIGHEST

def shifted(padded, which, offset):
    window = [slice(None), slice(None)]
    for place in (2, 3, 4):
        length = padded.shape[place]
        if place == which:
            window.append(slice(2 + offset, length - 2 + offset))
        else:
            window.append(slice(2, length - 2))
    return padded[tuple(window)]

def apply_operator(padded, mass):
    center = shifted(padded, 2, 0)
    nearby = jnp.zeros_like(center)
    farther = jnp.zeros_like(center)
    for which in (2, 3, 4):
        nearby = nearby + shifted(padded, which, 1) + shifted(padded, which, -1)
        farther = farther + shifted(padded, which, 2) + shifted(padded, which, -2)
    return (mass + 7.5) * center - 4.0 / 3.0 * nearby + 1.0 / 12.0 * farther

def spd_solve(matrix, rhs):
    lower = jnp.linalg.cholesky(matrix)
    middle = lax.linalg.triangular_solve(lower, rhs, left_side=True, lower=True)
    return lax.linalg.triangular_solve(lower, middle, left_side=True, lower=True, transpose_a=True)

def reference(solution, residual, direction, mass, coarse_basis, line_inverse, coarse_factor):
    directions = direction.shape[0]
    shape = direction.shape
    padded = jnp.pad(direction, ((0, 0), (0, 0), (2, 2), (2, 2), (2, 2)))
    image = apply_operator(padded, mass)
    flat_p = direction.reshape(directions, -1)
    flat_q = image.reshape(directions, -1)
    flat_r = residual.reshape(directions, -1)
    gram_pq = jnp.dot(flat_p, flat_q.T, precision=exact_mode)
    proj_pr = jnp.dot(flat_p, flat_r.T, precision=exact_mode)
    alpha_mix = spd_solve(gram_pq, proj_pr)
    new_solution = solution + jnp.dot(alpha_mix.T, flat_p, precision=exact_mode).reshape(shape)
    flat_new = flat_r - jnp.dot(alpha_mix.T, flat_q, precision=exact_mode)
    new_residual = flat_new.reshape(shape)
    blocked = new_residual.reshape(directions, 3, N_SUB, CX, N_INNER, CY, NZ)
    basis_blocked = coarse_basis.reshape(NB, 3, N_SUB, CX, N_INNER, CY, NZ)
    local_part = jnp.einsum('abzw,kcaxbyw->kcaxbyz', line_inverse, blocked, precision=exact_mode)
    coarse_rhs = jnp.einsum('jcaxbyz,kcaxbyz->abjk', basis_blocked, blocked, precision=exact_mode)
    coarse_rhs = coarse_rhs.reshape(NB * N_SUB * N_INNER, directions)
    coarse_mid = jnp.dot(coarse_factor.T, coarse_rhs, precision=exact_mode)
    coarse_sol = jnp.dot(coarse_factor, coarse_mid, precision=exact_mode)
    coarse_sol = coarse_sol.reshape(N_SUB, N_INNER, NB, directions)
    correction = jnp.einsum('jcaxbyz,abjk->kcaxbyz', basis_blocked, coarse_sol, precision=exact_mode)
    precond = (local_part + correction).reshape(directions, -1)
    cross_qz = jnp.dot(flat_q, precond.T, precision=exact_mode)
    beta_mix = -spd_solve(gram_pq, cross_qz)
    new_direction = (precond + jnp.dot(beta_mix.T, flat_p, precision=exact_mode)).reshape(shape)
    return (new_solution, new_residual, new_direction)
```

```python
import functools

import jax
import jax.numpy as jnp
from jax import lax
from jax.experimental import pallas as pl
from jax.experimental.pallas import tpu as pltpu
from jax.sharding import PartitionSpec as P

MESH = pl.DeviceIdType.MESH
EXACT = lax.Precision.HIGHEST
CLOSE = lax.Precision.HIGH
F32 = jnp.float32
WIDTH = 2
TILE = 8


def dot(a, b, precision):
    return lax.dot_general(a, b, (((1,), (0,)), ((), ())), precision=precision, preferred_element_type=F32)


def dot_t(a, b, precision):
    return lax.dot_general(a, b, (((1,), (1,)), ((), ())), precision=precision, preferred_element_type=F32)


def inverse_cholesky(gram):
    size = gram.shape[0]
    rows = lax.broadcasted_iota(jnp.int32, (size, size), 0)
    columns = lax.broadcasted_iota(jnp.int32, (size, size), 1)
    work = jnp.concatenate([gram, (rows == columns).astype(F32)], axis=1)
    below = lax.broadcasted_iota(jnp.int32, work.shape, 0)
    for j in range(size):
        scale = lax.rsqrt(work[j : j + 1, j : j + 1])
        row = work[j : j + 1, :] * scale
        column = work[:, j : j + 1] * scale
        work = jnp.where(below > j, work - column * row, jnp.where(below == j, row, work))
    return work[:, size:]


def step_kernel(
    axes, sizes,
    p_hbm, r_hbm, s_hbm, b_hbm, mass_ref, line_ref, factor_ref,
    s_out, r_out, d_out,
    p_nat, r_nat, s_nat, b_nat, stack, image, resid, up, down, left, right,
    parts, landed, full, lined_flat,
    load_sem, send_sem, recv_sem, rs_send, rs_recv, ag_send, ag_recv,
):
    (sub_axis, inner_axis), (n_sub, n_inner) = axes, sizes
    n = n_sub * n_inner
    K, comps, nodes, cz = p_hbm.shape
    cy = TILE // WIDTH
    cx = nodes // cy
    M = comps * nodes
    span = M * cz
    chunk = nodes * cz
    NC = factor_ref.shape[1]
    S = parts.shape[1]
    sub, inner = lax.axis_index(sub_axis), lax.axis_index(inner_axis)
    me = sub * n_inner + inner
    LR, LQ, B, PP = (pl.ds(i * K, K) for i in range(4))

    def device(linear):
        return {sub_axis: linear // n_inner, inner_axis: linear % n_inner}

    loads = []
    for i, (src, dst) in enumerate(((p_hbm, p_nat), (r_hbm, r_nat), (b_hbm, b_nat), (s_hbm, s_nat))):
        loads.append(pltpu.make_async_copy(src, dst, load_sem.at[i]))
        loads[-1].start()

    barrier = pltpu.get_barrier_semaphore()
    for d in range(1, n):
        pl.semaphore_signal(barrier, inc=1, device_id=device((me + d) % n), device_id_type=MESH)
    pl.semaphore_wait(barrier, n - 1)

    def remote(src, dst, ssem, rsem, target):
        return pltpu.make_async_remote_copy(
            src_ref=src, dst_ref=dst, send_sem=ssem, recv_sem=rsem, device_id=target, device_id_type=MESH
        )

    edge = WIDTH * cy

    @pl.when(sub < n_sub - 1)
    def _():
        for c in range(comps):
            remote(p_hbm.at[:, c, pl.ds(nodes - edge, edge)], up.at[c], send_sem.at[0, c], recv_sem.at[0, c],
                   {sub_axis: sub + 1}).start()

    @pl.when(sub > 0)
    def _():
        for c in range(comps):
            remote(p_hbm.at[:, c, pl.ds(0, edge)], down.at[c], send_sem.at[1, c], recv_sem.at[1, c],
                   {sub_axis: sub - 1}).start()

    def tile_rows(nat, m):
        flat = nat.reshape(K * M, cz)
        return flat[pl.ds(m, K, stride=M), :]

    def lanes(m, count=1):
        return pl.ds(m * cz, count * cz)

    loads[0].wait()
    for m in range(M):
        stack[PP, lanes(m)] = tile_rows(p_nat, m)

    @pl.when(inner < n_inner - 1)
    def _():
        for c in range(comps):
            for x in range(cx):
                remote(stack.at[PP, lanes((c * cx + x) * cy + cy - WIDTH, WIDTH)],
                       left.at[:, lanes((c * cx + x) * WIDTH, WIDTH)],
                       send_sem.at[2, c], recv_sem.at[2, c], {inner_axis: inner + 1}).start()

    @pl.when(inner > 0)
    def _():
        for c in range(comps):
            for x in range(cx):
                remote(stack.at[PP, lanes((c * cx + x) * cy, WIDTH)],
                       right.at[:, lanes((c * cx + x) * WIDTH, WIDTH)],
                       send_sem.at[3, c], recv_sem.at[3, c], {inner_axis: inner - 1}).start()

    @pl.when(sub == 0)
    def _():
        up[...] = jnp.zeros_like(up)

    @pl.when(sub == n_sub - 1)
    def _():
        down[...] = jnp.zeros_like(down)

    @pl.when(inner == 0)
    def _():
        left[...] = jnp.zeros_like(left)

    @pl.when(inner == n_inner - 1)
    def _():
        right[...] = jnp.zeros_like(right)

    line = line_ref[...]
    loads[1].wait()
    loads[2].wait()
    lined_flat[...] = dot_t(r_nat[...].reshape(K * M, cz), line, CLOSE)
    for m in range(M):
        stack[B, lanes(m)] = tile_rows(b_nat, m)
        resid[:, lanes(m)] = tile_rows(r_nat, m)
        stack[LR, lanes(m)] = lined_flat[pl.ds(m, K, stride=M), :]
    with_r = dot_t(resid[...], stack[pl.ds(2 * K, 2 * K), :], EXACT)

    lane = lax.broadcasted_iota(jnp.int32, (K, cz), 1)
    near, far = -4.0 / 3.0, 1.0 / 12.0

    def own(c, x, y):
        return stack[PP, lanes((c * cx + x) * cy + y)]

    for c in range(comps):
        for x in range(cx):
            for y in range(cy):
                centre = own(c, x, y)
                close, wide = [], []
                for off, group in ((1, close), (2, wide)):
                    group.append(jnp.where(lane >= off, pltpu.roll(centre, off, 1), 0.0))
                    group.append(jnp.where(lane < cz - off, pltpu.roll(centre, cz - off, 1), 0.0))
                    for sign in (off, -off):
                        if 0 <= x + sign < cx:
                            group.append(own(c, x + sign, y))
                        if 0 <= y + sign < cy:
                            group.append(own(c, x, y + sign))
                weight = mass_ref[pl.ds(x * cy + y, 1), :] + 7.5
                image[:, lanes((c * cx + x) * cy + y)] = (
                    weight * centre + near * functools.reduce(jnp.add, close) + far * functools.reduce(jnp.add, wide)
                )

    def wait_for(ref, sem):
        pltpu.make_async_copy(ref, ref, sem).wait()

    side = cx * WIDTH
    total = jnp.zeros((K, 4 * K), F32)
    for c in range(comps):
        @pl.when(sub > 0)
        def _():
            wait_for(up.at[c], recv_sem.at[0, c])

        @pl.when(sub < n_sub - 1)
        def _():
            wait_for(down.at[c], recv_sem.at[1, c])

        @pl.when(inner > 0)
        def _():
            wait_for(left.at[:, lanes(c * side, side)], recv_sem.at[2, c])

        @pl.when(inner < n_inner - 1)
        def _():
            wait_for(right.at[:, lanes(c * side, side)], recv_sem.at[3, c])

        above = up.at[c].reshape(K * edge, cz)
        under = down.at[c].reshape(K * edge, cz)

        def halo_tile(x, y):
            if x < 0:
                return above[pl.ds((x + WIDTH) * cy + y, K, stride=edge), :]
            if x >= cx:
                return under[pl.ds((x - cx) * cy + y, K, stride=edge), :]
            if y < 0:
                return left[:, lanes((c * cx + x) * WIDTH + y + WIDTH)]
            if y >= cy:
                return right[:, lanes((c * cx + x) * WIDTH + y - cy)]
            return None

        for x in range(cx):
            for y in range(cy):
                where = lanes((c * cx + x) * cy + y)
                value = image[:, where]
                for off, weight in ((1, near), (2, far)):
                    for sign in (off, -off):
                        for tile in (halo_tile(x + sign, y), halo_tile(x, y + sign)):
                            if tile is not None:
                                value = value + weight * tile
                image[:, where] = value

        tiles = jnp.concatenate([image[:, lanes(c * nodes + i)] for i in range(nodes)], axis=0)
        lined = dot_t(tiles, line, CLOSE)
        for i in range(nodes):
            stack[LQ, lanes(c * nodes + i)] = lined[i * K : (i + 1) * K]
        total = total + dot_t(image[:, pl.ds(c * chunk, chunk)], stack[:, pl.ds(c * chunk, chunk)], EXACT)

    both = jnp.concatenate([total[:, 2 * K : 3 * K], with_r[:, :K]], axis=0)
    mids = dot(both, factor_ref[...], EXACT)
    small = jnp.concatenate([total[:, : 2 * K], total[:, 3 * K :], with_r[:, K:]], axis=1)
    per_row = NC // cz
    for t in range(n):
        a, b = t // per_row, t % per_row
        for half in range(2):
            parts[t, pl.ds(half * TILE, TILE), :] = mids[
                half * K + a * TILE : half * K + (a + 1) * TILE, b * cz : (b + 1) * cz
            ]
    parts.reshape(n * S, cz)[pl.ds(2 * TILE, K, stride=S), :] = small

    for d in range(1, n):
        peer = (me + d) % n
        remote(parts.at[peer], landed.at[d], rs_send, rs_recv, device(peer)).start()
    wait_for(landed.at[pl.ds(1, n - 1)], rs_recv)
    mine = parts[me]
    for d in range(1, n):
        mine = mine + landed[d]
    full[me] = mine
    for d in range(1, n):
        remote(full.at[me], full.at[me], ag_send, ag_recv, device((me + d) % n)).start()
    wait_for(full.at[pl.ds(0, n - 1)], ag_recv)

    sums = full.reshape(n * S, cz)[pl.ds(2 * TILE, K, stride=S), :]
    lined_r_sum, lined_q_sum = sums[:, :K], sums[:, K : 2 * K]
    gram, proj_t = sums[:, 2 * K : 3 * K], sums[:, 3 * K :]
    mid = [
        jnp.concatenate(
            [
                jnp.concatenate([full[a * per_row + b, half * TILE : (half + 1) * TILE] for b in range(per_row)], axis=1)
                for a in range(K // TILE)
            ],
            axis=0,
        )
        for half in range(2)
    ]
    mid_q, mid_r = mid
    inv = inverse_cholesky(gram)

    def solve_t(rhs_t):
        return dot(dot_t(rhs_t, inv, EXACT), inv, EXACT)

    alpha_t = solve_t(proj_t)
    mid_new = mid_r - dot(alpha_t, mid_q, EXACT)
    last = dot_t(mid_new, jnp.concatenate([mid_q, factor_ref[...]], axis=0), EXACT)
    cross_t = lined_r_sum.T - dot_t(alpha_t, lined_q_sum, EXACT) + last[:, :K]
    beta_t = -solve_t(cross_t)
    mix = jnp.concatenate([-alpha_t, last[:, K:], beta_t], axis=1)

    loads[3].wait()
    s_flat = s_nat.reshape(K * M, cz)
    outs = [ref.reshape(K * M, cz) for ref in (s_out, r_out, d_out)]
    for c in range(comps):
        part = pl.ds(c * chunk, chunk)
        moved = dot(alpha_t, stack[PP, part], CLOSE)
        lowered = resid[:, part] - dot(alpha_t, image[:, part], CLOSE)
        turned = stack[LR, part] + dot(mix, stack[pl.ds(K, 3 * K), part], CLOSE)
        for i in range(nodes):
            rows = pl.ds(c * nodes + i, K, stride=M)
            cut = slice(i * cz, (i + 1) * cz)
            outs[0][rows, :] = s_flat[rows, :] + moved[:, cut]
            outs[1][rows, :] = lowered[:, cut]
            outs[2][rows, :] = turned[:, cut]

    for which, there, buffer in (
        (0, sub < n_sub - 1, up), (1, sub > 0, down), (2, inner < n_inner - 1, left), (3, inner > 0, right),
    ):
        @pl.when(there)
        def _(which=which, buffer=buffer):
            for c in range(comps):
                piece = buffer.at[c] if which < 2 else buffer.at[:, lanes(c * side, side)]
                wait_for(piece, send_sem.at[which, c])
    wait_for(landed.at[pl.ds(1, n - 1)], rs_send)
    wait_for(full.at[pl.ds(0, n - 1)], ag_send)


def on_device(axes, sizes, solution, residual, direction, mass, coarse_basis, line_inverse, coarse_factor):
    K, comps, cx, cy, cz = direction.shape
    n = sizes[0] * sizes[1]
    NC = coarse_factor.shape[1]
    nodes, M = cx * cy, comps * cx * cy
    assert K * NC == n * TILE * cz and K <= n and 4 * K <= cz and WIDTH * cy == TILE
    flat = (K, comps, nodes, cz)
    S = 3 * TILE
    vmem = pl.BlockSpec(memory_space=pltpu.VMEM)
    hbm = pl.BlockSpec(memory_space=pl.ANY)
    dma = pltpu.SemaphoreType.DMA
    natural = pltpu.VMEM(flat, F32)
    wide = pltpu.VMEM((K, M * cz), F32)
    outs = pl.pallas_call(
        functools.partial(step_kernel, axes, sizes),
        out_shape=[jax.ShapeDtypeStruct(flat, F32)] * 3,
        in_specs=[hbm] * 4 + [vmem] * 3,
        out_specs=[vmem] * 3,
        scratch_shapes=[
            natural, natural, natural, natural,
            pltpu.VMEM((4 * K, M * cz), F32), wide, wide,
            pltpu.VMEM((comps, K, WIDTH * cy, cz), F32), pltpu.VMEM((comps, K, WIDTH * cy, cz), F32),
            pltpu.VMEM((K, comps * cx * WIDTH * cz), F32), pltpu.VMEM((K, comps * cx * WIDTH * cz), F32),
            pltpu.VMEM((n, S, cz), F32), pltpu.VMEM((n, S, cz), F32), pltpu.VMEM((n, S, cz), F32),
            pltpu.VMEM((K * M, cz), F32),
            dma((4,)), dma((4, comps)), dma((4, comps)), dma, dma, dma, dma,
        ],
        compiler_params=pltpu.CompilerParams(collective_id=0, has_side_effects=True, vmem_limit_bytes=48 << 20),
    )(
        direction.reshape(flat), residual.reshape(flat), solution.reshape(flat), coarse_basis.reshape(flat),
        mass.reshape(nodes, cz), line_inverse.reshape(cz, cz), coarse_factor,
    )
    return tuple(out.reshape(direction.shape) for out in outs)


def solution(mesh):
    axes = tuple(mesh.axis_names)
    sizes = tuple(mesh.shape[a] for a in axes)
    sub, inner = axes
    field = P(None, None, sub, inner, None)
    return jax.shard_map(
        functools.partial(on_device, axes, sizes),
        mesh=mesh,
        in_specs=(field, field, field, P(sub, inner, None), field, P(sub, inner, None, None), P((sub, inner), None)),
        out_specs=(field, field, field),
        check_vma=False,
    )
```

```python
import functools

import jax
import jax.numpy as jnp
from jax import lax
from jax.experimental import pallas as pl
from jax.experimental.pallas import tpu as pltpu
from jax.sharding import PartitionSpec as P

MESH = pl.DeviceIdType.MESH
EXACT = lax.Precision.HIGHEST
CLOSE = lax.Precision.HIGH
F32 = jnp.float32
BF16 = jnp.bfloat16
WIDTH = 2
TILE = 8
SLOT = 2 * TILE
USED = TILE + 1


def dot(a, b, precision=None):
    return lax.dot_general(a, b, (((1,), (0,)), ((), ())), precision=precision, preferred_element_type=F32)


def dot_t(a, b, precision=None):
    return lax.dot_general(a, b, (((1,), (1,)), ((), ())), precision=precision, preferred_element_type=F32)


def split(x):
    high = x.astype(BF16)
    return high, (x - high.astype(F32)).astype(BF16)


def fold(x, rows):
    return x[:rows] + x[rows:]


def four_lanes(x):
    high, low = split(x)
    return jnp.concatenate([high, low, high, low], axis=1)


def four_rows(x):
    high, low = split(x)
    return jnp.concatenate([high, high, low, low], axis=0)


def inverse_cholesky(gram):
    size = gram.shape[0]
    rows = lax.broadcasted_iota(jnp.int32, (size, size), 0)
    columns = lax.broadcasted_iota(jnp.int32, (size, size), 1)
    work = jnp.concatenate([gram, (rows == columns).astype(F32)], axis=1)
    below = lax.broadcasted_iota(jnp.int32, work.shape, 0)
    for j in range(size):
        scale = lax.rsqrt(work[j : j + 1, j : j + 1])
        row = work[j : j + 1, :] * scale
        column = work[:, j : j + 1] * scale
        work = jnp.where(below > j, work - column * row, jnp.where(below == j, row, work))
    return work[:, size:]


def step_kernel(
    axes, sizes,
    p_hbm, r_hbm, s_hbm, b_hbm, mass_hbm, line_hbm, factor_hbm,
    s_out, r_out, d_out,
    p_nat, r_nat, s_nat, b_nat, field, image, xb, qb, rb, fb, up, down, left, right,
    early_parts, early_landed, early_full, parts, landed, full, mass_ref, line_ref, factor_ref,
    load_sem, send_sem, recv_sem, sum_sem,
):
    (sub_axis, inner_axis), (n_sub, n_inner) = axes, sizes
    n = n_sub * n_inner
    K, comps, nodes, cz = p_hbm.shape
    cy = TILE // WIDTH
    cx = nodes // cy
    M = comps * nodes
    chunk = nodes * cz
    NC = factor_hbm.shape[1]
    per_row = NC // cz
    edge = WIDTH * cy
    side = cx * WIDTH
    sub, inner = lax.axis_index(sub_axis), lax.axis_index(inner_axis)
    me = sub * n_inner + inner
    LR, LQ, B, PP = 0, K, 4 * K, 5 * K
    LOW = 2 * K

    loads = []
    for i, (src, dst) in enumerate((
        (p_hbm, p_nat), (r_hbm, r_nat), (line_hbm, line_ref), (b_hbm, b_nat), (mass_hbm, mass_ref),
        (factor_hbm, factor_ref), (s_hbm, s_nat),
    )):
        loads.append(pltpu.make_async_copy(src, dst, load_sem.at[i]))
        loads[-1].start()

    subs, inners = [sub], [inner]
    for d in range(1, n_sub):
        subs.append(jnp.where(sub + d < n_sub, sub + d, sub + d - n_sub))
    for d in range(1, n_inner):
        inners.append(jnp.where(inner + d < n_inner, inner + d, inner + d - n_inner))
    peers = [
        (i * n_inner + j, a * n_inner + b, {sub_axis: a, inner_axis: b})
        for i, a in enumerate(subs) for j, b in enumerate(inners) if i or j
    ]

    barrier = pltpu.get_barrier_semaphore()
    for _, _, target in peers:
        pl.semaphore_signal(barrier, inc=1, device_id=target, device_id_type=MESH)
    pl.semaphore_wait(barrier, n - 1)

    def remote(src, dst, ssem, rsem, target):
        return pltpu.make_async_remote_copy(
            src_ref=src, dst_ref=dst, send_sem=ssem, recv_sem=rsem, device_id=target, device_id_type=MESH
        )

    def wait_for(ref, sem):
        pltpu.make_async_copy(ref, ref, sem).wait()

    def lanes(m, count=1):
        return pl.ds(m * cz, count * cz)

    def tile_rows(nat, m):
        return nat.reshape(K * M, cz)[pl.ds(m, K, stride=M), :]

    def put(ref, row, distance, where, value):
        high, low = split(value)
        ref[pl.ds(row, K), where] = high
        ref[pl.ds(row + distance, K), where] = low

    @pl.when(sub < n_sub - 1)
    def _():
        for c in range(comps):
            remote(p_hbm.at[:, c, pl.ds(nodes - edge, edge)], up.at[c], send_sem.at[0, c], recv_sem.at[0, c],
                   {sub_axis: sub + 1}).start()

    loads[0].wait()
    for m in range(M):
        field[:, lanes(m)] = tile_rows(p_nat, m)

    @pl.when(inner < n_inner - 1)
    def _():
        for c in range(comps):
            for x in range(cx):
                remote(field.at[:, lanes((c * cx + x) * cy + cy - WIDTH, WIDTH)],
                       left.at[:, lanes((c * cx + x) * WIDTH, WIDTH)],
                       send_sem.at[2, c], recv_sem.at[2, c], {inner_axis: inner + 1}).start()

    @pl.when(inner > 0)
    def _():
        for c in range(comps):
            for x in range(cx):
                remote(field.at[:, lanes((c * cx + x) * cy, WIDTH)],
                       right.at[:, lanes((c * cx + x) * WIDTH, WIDTH)],
                       send_sem.at[3, c], recv_sem.at[3, c], {inner_axis: inner - 1}).start()

    for buffer, alone in (
        (up, sub == 0), (down, sub == n_sub - 1), (left, inner == 0), (right, inner == n_inner - 1),
    ):
        @pl.when(alone)
        def _(buffer=buffer):
            buffer[...] = jnp.zeros_like(buffer)

    for load in loads[1:]:
        load.wait()
    for m in range(M):
        put(rb, 0, K, lanes(m), tile_rows(r_nat, m))
        put(xb, B, LOW, lanes(m), tile_rows(b_nat, m))
        put(xb, PP, LOW, lanes(m), field[:, lanes(m)])
    fh, fl = split(factor_ref[...])
    for i, half in enumerate((fh, fh, fl, fl)):
        fb[pl.ds(i * K, K), :] = half

    with_r = jnp.zeros((2 * K, 4 * K), F32)
    for c in range(comps):
        part = pl.ds(c * chunk, chunk)
        with_r = with_r + dot_t(rb[:, part], xb[pl.ds(B, 4 * K), part])
    with_r = fold(with_r, K)
    with_r = with_r[:, :LOW] + with_r[:, LOW:]

    def spread(mid, small, slots):
        for t in range(n):
            a, b = t // per_row, t % per_row
            slots[t, pl.ds(0, TILE), :] = mid[a * TILE : (a + 1) * TILE, b * cz : (b + 1) * cz]
        slots.reshape(n * SLOT, cz)[pl.ds(TILE, K, stride=SLOT), :] = small

    def scatter(slots, arriving, ssem, rsem):
        for d, peer, target in peers:
            remote(slots.at[peer, pl.ds(0, USED)], arriving.at[d, pl.ds(0, USED)], ssem, rsem, target).start()

    def gather(slots, arriving, whole, rsem, ssem, next_rsem):
        wait_for(arriving.at[pl.ds(1, n - 1), pl.ds(0, USED)], rsem)
        for rows in (pl.ds(0, TILE), pl.ds(TILE, 1)):
            mine = slots[me, rows]
            for d in range(1, n):
                mine = mine + arriving[d, rows]
            whole[me, rows] = mine
        for _, _, target in peers:
            remote(whole.at[me, pl.ds(0, USED)], whole.at[me, pl.ds(0, USED)], ssem, next_rsem, target).start()

    def collect(whole, rsem):
        wait_for(whole.at[pl.ds(0, n - 1), pl.ds(0, USED)], rsem)
        mid = jnp.concatenate(
            [
                jnp.concatenate([whole[a * per_row + b, pl.ds(0, TILE)] for b in range(per_row)], axis=1)
                for a in range(K // TILE)
            ],
            axis=0,
        )
        return mid, whole.reshape(n * SLOT, cz)[pl.ds(TILE, K, stride=SLOT), :]

    spread(
        dot(four_lanes(with_r[:, :K]), fb[...]),
        jnp.concatenate([with_r[:, K:], jnp.zeros((K, cz - K), F32)], axis=1),
        early_parts,
    )
    scatter(early_parts, early_landed, sum_sem.at[0], sum_sem.at[1])

    @pl.when(sub > 0)
    def _():
        for c in range(comps):
            remote(p_hbm.at[:, c, pl.ds(0, edge)], down.at[c], send_sem.at[1, c], recv_sem.at[1, c],
                   {sub_axis: sub - 1}).start()

    line_high, line_low = split(line_ref[...])
    line_both = jnp.concatenate([line_high, line_high], axis=1)

    def lined(source, c):
        high = jnp.concatenate([source[pl.ds(0, K), lanes(c * nodes + i)] for i in range(nodes)], axis=0)
        low = jnp.concatenate([source[pl.ds(K, K), lanes(c * nodes + i)] for i in range(nodes)], axis=0)
        return dot_t(jnp.concatenate([high, low], axis=1), line_both) + dot_t(high, line_low)

    lane = lax.broadcasted_iota(jnp.int32, (K, cz), 1)
    near, far = -4.0 / 3.0, 1.0 / 12.0

    def own(c, x, y):
        return field[:, lanes((c * cx + x) * cy + y)]

    for c in range(comps):
        turned = lined(rb, c)
        for i in range(nodes):
            put(xb, LR, LOW, lanes(c * nodes + i), turned[i * K : (i + 1) * K])
        for x in range(cx):
            for y in range(cy):
                centre = own(c, x, y)
                close, wide = [], []
                for off, group in ((1, close), (2, wide)):
                    group.append(jnp.where(lane >= off, pltpu.roll(centre, off, 1), 0.0))
                    group.append(jnp.where(lane < cz - off, pltpu.roll(centre, cz - off, 1), 0.0))
                    for sign in (off, -off):
                        if 0 <= x + sign < cx:
                            group.append(own(c, x + sign, y))
                        if 0 <= y + sign < cy:
                            group.append(own(c, x, y + sign))
                weight = mass_ref[pl.ds(x * cy + y, 1), :] + 7.5
                image[:, lanes((c * cx + x) * cy + y)] = (
                    weight * centre + near * functools.reduce(jnp.add, close) + far * functools.reduce(jnp.add, wide)
                )

    gather(early_parts, early_landed, early_full, sum_sem.at[1], sum_sem.at[2], sum_sem.at[3])

    total = jnp.zeros((2 * K, 8 * K), F32)
    for c in range(comps):
        for which, (there, piece) in enumerate((
            (sub > 0, up.at[c]), (sub < n_sub - 1, down.at[c]),
            (inner > 0, left.at[:, lanes(c * side, side)]), (inner < n_inner - 1, right.at[:, lanes(c * side, side)]),
        )):
            @pl.when(there)
            def _(which=which, piece=piece):
                wait_for(piece, recv_sem.at[which, c])

        above = up.at[c].reshape(K * edge, cz)
        under = down.at[c].reshape(K * edge, cz)

        def halo_tile(x, y):
            if x < 0:
                return above[pl.ds((x + WIDTH) * cy + y, K, stride=edge), :]
            if x >= cx:
                return under[pl.ds((x - cx) * cy + y, K, stride=edge), :]
            if y < 0:
                return left[:, lanes((c * cx + x) * WIDTH + y + WIDTH)]
            if y >= cy:
                return right[:, lanes((c * cx + x) * WIDTH + y - cy)]
            return None

        for x in range(cx):
            for y in range(cy):
                where = lanes((c * cx + x) * cy + y)
                value = image[:, where]
                for off, weight in ((1, near), (2, far)):
                    for sign in (off, -off):
                        for tile in (halo_tile(x + sign, y), halo_tile(x, y + sign)):
                            if tile is not None:
                                value = value + weight * tile
                put(qb, 0, K, where, value)

        turned = lined(qb, c)
        for i in range(nodes):
            put(xb, LQ, LOW, lanes(c * nodes + i), turned[i * K : (i + 1) * K])
        part = pl.ds(c * chunk, chunk)
        total = total + dot_t(qb[:, part], xb[:, part])

    total = fold(total, K)
    lines_q = total[:, :LOW] + total[:, LOW : 2 * LOW]
    rest_q = total[:, 2 * LOW : 3 * LOW] + total[:, 3 * LOW :]
    spread(
        dot(four_lanes(rest_q[:, :K]), fb[...]),
        jnp.concatenate([lines_q, rest_q[:, K:], jnp.zeros((K, cz - 3 * K), F32)], axis=1),
        parts,
    )
    scatter(parts, landed, sum_sem.at[4], sum_sem.at[5])
    gather(parts, landed, full, sum_sem.at[5], sum_sem.at[6], sum_sem.at[7])
    mid_r, sums_r = collect(early_full, sum_sem.at[3])
    mid_q, sums_q = collect(full, sum_sem.at[7])

    inv = inverse_cholesky(sums_q[:, 2 * K : 3 * K])

    def solve_t(rhs_t):
        return dot(dot_t(rhs_t, inv, EXACT), inv, EXACT)

    alpha_t = solve_t(sums_r[:, :K])
    mid_new = mid_r - dot(four_lanes(alpha_t), four_rows(mid_q))
    last = fold(dot_t(
        jnp.concatenate(split(mid_new), axis=0),
        jnp.concatenate([*split(mid_q), fb[pl.ds(0, K), :], fb[pl.ds(2 * K, K), :]], axis=0),
    ), K)
    crossed, coarse_t = last[:, :K] + last[:, K : 2 * K], last[:, 2 * K : 3 * K] + last[:, 3 * K :]
    cross_t = sums_q[:, :K].T - dot_t(alpha_t, sums_q[:, K : 2 * K], EXACT) + crossed
    beta_t = -solve_t(cross_t)

    (ah, al), (bh, bl), (ch, cl) = split(alpha_t), split(beta_t), split(coarse_t)
    none = jnp.zeros((K, K), BF16)
    unit = (lax.broadcasted_iota(jnp.int32, (K, K), 0) == lax.broadcasted_iota(jnp.int32, (K, K), 1)).astype(BF16)

    def table(rows):
        return jnp.concatenate([jnp.concatenate(row, axis=1) for row in rows], axis=0)

    on_fields = table([[ch, bh, ch, bh], [cl, bl, none, none], [none, ah, none, ah], [none, al, none, none]])
    on_lines = table([[unit, -ah, unit, -ah], [none, -al, none, none]])
    on_image = table([[ah, ah], [al, none]])

    s_flat, r_flat = (nat.reshape(K * M, cz) for nat in (s_nat, r_nat))
    outs = [ref.reshape(K * M, cz) for ref in (s_out, r_out, d_out)]
    for c in range(comps):
        part = pl.ds(c * chunk, chunk)
        mixed = dot(on_fields, xb[pl.ds(B, 4 * K), part])
        turned = fold(mixed[: 2 * K], K) + fold(dot(on_lines, xb[pl.ds(0, 4 * K), part]), K)
        moved = fold(mixed[2 * K :], K)
        drop = fold(dot(on_image, qb[:, part]), K)
        for i in range(nodes):
            rows = pl.ds(c * nodes + i, K, stride=M)
            cut = slice(i * cz, (i + 1) * cz)
            outs[0][rows, :] = s_flat[rows, :] + moved[:, cut]
            outs[1][rows, :] = r_flat[rows, :] - drop[:, cut]
            outs[2][rows, :] = turned[:, cut]

    for which, there, buffer in (
        (0, sub < n_sub - 1, up), (1, sub > 0, down), (2, inner < n_inner - 1, left), (3, inner > 0, right),
    ):
        @pl.when(there)
        def _(which=which, buffer=buffer):
            for c in range(comps):
                piece = buffer.at[c] if which < 2 else buffer.at[:, lanes(c * side, side)]
                wait_for(piece, send_sem.at[which, c])
    for i in (0, 2, 4, 6):
        wait_for(full.at[pl.ds(0, n - 1), pl.ds(0, USED)], sum_sem.at[i])


def write_kernel(*refs):
    count = len(refs) // 2
    sources, targets, sem = refs[:count], refs[count : 2 * count], refs[-1]
    copies = [pltpu.make_async_copy(a, b, sem.at[i]) for i, (a, b) in enumerate(zip(sources, targets))]
    for copy in copies:
        copy.start()
    for copy in copies:
        copy.wait()


def on_device(axes, sizes, solution, residual, direction, mass, coarse_basis, line_inverse, coarse_factor):
    K, comps, cx, cy, cz = direction.shape
    n = sizes[0] * sizes[1]
    NC = coarse_factor.shape[1]
    nodes, M = cx * cy, comps * cx * cy
    assert K * NC == n * TILE * cz and K <= n and 4 * K <= cz and WIDTH * cy == TILE
    flat = (K, comps, nodes, cz)
    vmem = pl.BlockSpec(memory_space=pltpu.VMEM)
    hbm = pl.BlockSpec(memory_space=pltpu.HBM)
    dma = pltpu.SemaphoreType.DMA
    natural = pltpu.VMEM(flat, F32)
    wide = pltpu.VMEM((K, M * cz), F32)
    across = pltpu.VMEM((comps, K, WIDTH * cy, cz), F32)
    beside = pltpu.VMEM((K, comps * cx * WIDTH * cz), F32)
    slots = pltpu.VMEM((n, SLOT, cz), F32)
    inputs = (
        direction.reshape(flat), residual.reshape(flat), solution.reshape(flat), coarse_basis.reshape(flat),
        mass.reshape(nodes, cz), line_inverse.reshape(cz, cz), coarse_factor,
    )
    outs = pl.pallas_call(
        functools.partial(step_kernel, axes, sizes),
        out_shape=[jax.ShapeDtypeStruct(flat, F32)] * 3,
        in_specs=[hbm] * 7,
        out_specs=[vmem] * 3,
        scratch_shapes=[
            natural, natural, natural, natural, wide, wide,
            pltpu.VMEM((8 * K, M * cz), BF16), pltpu.VMEM((2 * K, M * cz), BF16), pltpu.VMEM((2 * K, M * cz), BF16),
            pltpu.VMEM((4 * K, NC), BF16),
            across, across, beside, beside,
            slots, slots, slots, slots, slots, slots,
            pltpu.VMEM((nodes, cz), F32), pltpu.VMEM((cz, cz), F32), pltpu.VMEM(coarse_factor.shape, F32),
            dma((7,)), dma((4, comps)), dma((4, comps)), dma((8,)),
        ],
        compiler_params=pltpu.CompilerParams(collective_id=0, has_side_effects=True, vmem_limit_bytes=48 << 20),
    )(*[pltpu.with_memory_space_constraint(array, pltpu.HBM) for array in inputs])
    outs = pl.pallas_call(
        write_kernel,
        out_shape=[jax.ShapeDtypeStruct(flat, F32)] * 3,
        in_specs=[vmem] * 3,
        out_specs=[hbm] * 3,
        scratch_shapes=[dma((3,))],
        compiler_params=pltpu.CompilerParams(vmem_limit_bytes=1 << 20),
    )(*outs)
    return tuple(out.reshape(direction.shape) for out in outs)


def solution(mesh):
    axes = tuple(mesh.axis_names)
    sizes = tuple(mesh.shape[a] for a in axes)
    sub, inner = axes
    field = P(None, None, sub, inner, None)
    return jax.shard_map(
        functools.partial(on_device, axes, sizes),
        mesh=mesh,
        in_specs=(field, field, field, P(sub, inner, None), field, P(sub, inner, None, None), P((sub, inner), None)),
        out_specs=(field, field, field),
        check_vma=False,
    )
```

```python
import functools

import jax
import jax.numpy as jnp
from jax import lax
from jax.experimental import pallas as pl
from jax.experimental.pallas import tpu as pltpu
from jax.sharding import PartitionSpec as P

MESH = pl.DeviceIdType.MESH
EXACT = lax.Precision.HIGHEST
CLOSE = lax.Precision.HIGH
F32 = jnp.float32
BF16 = jnp.bfloat16
WIDTH = 2
TILE = 8
SLOT = 2 * TILE
USED = TILE + 1


def dot(a, b, precision=None):
    return lax.dot_general(a, b, (((1,), (0,)), ((), ())), precision=precision, preferred_element_type=F32)


def dot_t(a, b, precision=None):
    return lax.dot_general(a, b, (((1,), (1,)), ((), ())), precision=precision, preferred_element_type=F32)


def split(x):
    high = x.astype(BF16)
    return high, (x - high.astype(F32)).astype(BF16)


def fold(x, rows):
    return x[:rows] + x[rows:]


def four_lanes(x):
    high, low = split(x)
    return jnp.concatenate([high, low, high, low], axis=1)


def four_rows(x):
    high, low = split(x)
    return jnp.concatenate([high, high, low, low], axis=0)


def inverse_cholesky(gram):
    size = gram.shape[0]
    rows = lax.broadcasted_iota(jnp.int32, (size, size), 0)
    columns = lax.broadcasted_iota(jnp.int32, (size, size), 1)
    work = jnp.concatenate([gram, (rows == columns).astype(F32)], axis=1)
    below = lax.broadcasted_iota(jnp.int32, work.shape, 0)
    for j in range(size):
        scale = lax.rsqrt(work[j : j + 1, j : j + 1])
        row = work[j : j + 1, :] * scale
        column = work[:, j : j + 1] * scale
        work = jnp.where(below > j, work - column * row, jnp.where(below == j, row, work))
    return work[:, size:]


def step_kernel(
    axes, sizes,
    p_hbm, r_hbm, s_hbm, b_hbm, mass_hbm, line_hbm, factor_hbm,
    s_out, r_out, d_out,
    p_nat, r_nat, s_nat, b_nat, field, image, xb, qb, rb, fb, up, down, left, right,
    early, early_a, held, early_b, early_full, parts, landed, full, mass_ref, line_ref, factor_ref,
    load_sem, send_sem, recv_sem, sum_sem, ready_sem,
):
    (sub_axis, inner_axis), (n_sub, n_inner) = axes, sizes
    n = n_sub * n_inner
    K, comps, nodes, cz = p_hbm.shape
    cy = TILE // WIDTH
    cx = nodes // cy
    M = comps * nodes
    chunk = nodes * cz
    NC = factor_hbm.shape[1]
    per_row = NC // cz
    edge = WIDTH * cy
    side = cx * WIDTH
    sub, inner = lax.axis_index(sub_axis), lax.axis_index(inner_axis)
    me = inner * n_sub + sub
    LR, LQ, B, PP = 0, K, 4 * K, 6 * K
    travel = pl.ds(0, USED)

    loads = []
    for i, (src, dst) in enumerate((
        (p_hbm, p_nat), (r_hbm, r_nat), (line_hbm, line_ref), (b_hbm, b_nat), (mass_hbm, mass_ref),
        (factor_hbm, factor_ref), (s_hbm, s_nat),
    )):
        loads.append(pltpu.make_async_copy(src, dst, load_sem.at[i]))
        loads[-1].start()

    def around(index, count):
        return [index] + [jnp.where(index + d < count, index + d, index + d - count) for d in range(1, count)]

    subs, inners = around(sub, n_sub), around(inner, n_inner)
    lines = ((sub_axis, sub, n_sub), (inner_axis, inner, n_inner))

    def greet(sem_of, reach):
        for which, (axis, index, count) in enumerate(lines):
            if reach < count:
                @pl.when(index + reach < count)
                def _():
                    pl.semaphore_signal(sem_of(which), inc=1, device_id={axis: index + reach}, device_id_type=MESH)

                @pl.when(index >= reach)
                def _():
                    pl.semaphore_signal(sem_of(which), inc=1, device_id={axis: index - reach}, device_id_type=MESH)

    def heard(index, count, reach):
        return (index + reach < count).astype(jnp.int32) + (index >= reach).astype(jnp.int32)

    barrier = pltpu.get_barrier_semaphore()
    greet(lambda which: barrier, 1)
    pl.semaphore_wait(barrier, heard(sub, n_sub, 1) + heard(inner, n_inner, 1))

    rounds = []
    reach = 1
    while reach < max(n_sub, n_inner) - 1:
        rounds.append(reach)
        reach *= 2

    def listen(step):
        for which, (axis, index, count) in enumerate(lines):
            if rounds[step] < count - 1:
                pl.semaphore_wait(ready_sem.at[which, step], heard(index, count, rounds[step]))

    def say(step):
        for which, (axis, index, count) in enumerate(lines):
            if rounds[step] < count - 1:
                @pl.when(index + rounds[step] < count)
                def _():
                    pl.semaphore_signal(ready_sem.at[which, step], inc=1, device_id={axis: index + rounds[step]},
                                        device_id_type=MESH)

                @pl.when(index >= rounds[step])
                def _():
                    pl.semaphore_signal(ready_sem.at[which, step], inc=1, device_id={axis: index - rounds[step]},
                                        device_id_type=MESH)

    spoken = [0]

    def advance(last=False):
        while spoken[0] < len(rounds):
            listen(spoken[0])
            spoken[0] += 1
            if spoken[0] < len(rounds):
                say(spoken[0])
            if not last:
                break

    def remote(src, dst, ssem, rsem, target):
        return pltpu.make_async_remote_copy(
            src_ref=src, dst_ref=dst, send_sem=ssem, recv_sem=rsem, device_id=target, device_id_type=MESH
        )

    def wait_for(ref, sem):
        pltpu.make_async_copy(ref, ref, sem).wait()

    def lanes(m, count=1):
        return pl.ds(m * cz, count * cz)

    def tile_rows(nat, m):
        return nat.reshape(K * M, cz)[pl.ds(m, K, stride=M), :]

    def put(ref, row, distance, where, value):
        high, low = split(value)
        ref[pl.ds(row, K), where] = high
        ref[pl.ds(row + distance, K), where] = low

    @pl.when(sub < n_sub - 1)
    def _():
        for c in range(comps):
            remote(p_hbm.at[:, c, pl.ds(nodes - edge, edge)], up.at[c], send_sem.at[0, c], recv_sem.at[0, c],
                   {sub_axis: sub + 1}).start()

    def send_down(some):
        @pl.when(sub > 0)
        def _():
            for c in some:
                remote(p_hbm.at[:, c, pl.ds(0, edge)], down.at[c], send_sem.at[1, c], recv_sem.at[1, c],
                       {sub_axis: sub - 1}).start()

    if rounds:
        say(0)
    loads[0].wait()
    for m in range(M):
        value = tile_rows(p_nat, m)
        field[:, lanes(m)] = value
        put(xb, PP, K, lanes(m), value)

    @pl.when(inner < n_inner - 1)
    def _():
        for c in range(comps):
            for x in range(cx):
                remote(field.at[:, lanes((c * cx + x) * cy + cy - WIDTH, WIDTH)],
                       left.at[:, lanes((c * cx + x) * WIDTH, WIDTH)],
                       send_sem.at[2, c], recv_sem.at[2, c], {inner_axis: inner + 1}).start()

    @pl.when(inner > 0)
    def _():
        for c in range(comps):
            for x in range(cx):
                remote(field.at[:, lanes((c * cx + x) * cy, WIDTH)],
                       right.at[:, lanes((c * cx + x) * WIDTH, WIDTH)],
                       send_sem.at[3, c], recv_sem.at[3, c], {inner_axis: inner - 1}).start()

    for buffer, alone in (
        (up, sub == 0), (down, sub == n_sub - 1), (left, inner == 0), (right, inner == n_inner - 1),
    ):
        @pl.when(alone)
        def _(buffer=buffer):
            buffer[...] = jnp.zeros_like(buffer)

    for load in loads[1:]:
        load.wait()
    advance()
    for m in range(M):
        put(rb, 0, K, lanes(m), tile_rows(r_nat, m))
        put(xb, B, K, lanes(m), tile_rows(b_nat, m))
    fh, fl = split(factor_ref[...])
    for i, half in enumerate((fh, fh, fl, fl)):
        fb[pl.ds(i * K, K), :] = half
    advance()

    def pairs(x):
        x = x[:, :K] + x[:, K:]
        return [x[i : i + K] + x[i + K : i + 2 * K] for i in range(0, x.shape[0], 2 * K)]

    with_r = jnp.zeros((4 * K, 2 * K), F32)
    for c in range(comps):
        part = pl.ds(c * chunk, chunk)
        with_r = with_r + dot_t(xb[pl.ds(B, 4 * K), part], rb[:, part])
    rhs_r, proj = pairs(with_r)

    def spread(mid, small, slots):
        for t in range(n):
            a, b = t // per_row, t % per_row
            slots[t, pl.ds(0, TILE), :] = mid[a * TILE : (a + 1) * TILE, b * cz : (b + 1) * cz]
        slots.reshape(n * SLOT, cz)[pl.ds(TILE, K, stride=SLOT), :] = small

    def collect(whole):
        mid = jnp.concatenate(
            [
                jnp.concatenate([whole[a * per_row + b, pl.ds(0, TILE)] for b in range(per_row)], axis=1)
                for a in range(K // TILE)
            ],
            axis=0,
        )
        return mid, whole.reshape(n * SLOT, cz)[pl.ds(TILE, K, stride=SLOT), :]

    line_high, line_low = split(line_ref[...])
    line_both = jnp.concatenate([line_high, line_high], axis=1)

    def lined(source, c):
        high = jnp.concatenate([source[pl.ds(0, K), lanes(c * nodes + i)] for i in range(nodes)], axis=0)
        low = jnp.concatenate([source[pl.ds(K, K), lanes(c * nodes + i)] for i in range(nodes)], axis=0)
        return dot_t(jnp.concatenate([high, low], axis=1), line_both) + dot_t(high, line_low)

    lane = lax.broadcasted_iota(jnp.int32, (K, cz), 1)
    near, far = -4.0 / 3.0, 1.0 / 12.0

    def own(c, x, y):
        return field[:, lanes((c * cx + x) * cy + y)]

    def against_field(c):
        part = pl.ds(c * chunk, chunk)
        return dot_t(xb[pl.ds(PP, 2 * K), part], qb[:, part])

    inside = jnp.zeros((2 * K, 2 * K), F32)
    for c in range(comps):
        turned = lined(rb, c)
        for i in range(nodes):
            put(xb, LR, 2 * K, lanes(c * nodes + i), turned[i * K : (i + 1) * K])
        for x in range(cx):
            for y in range(cy):
                centre = own(c, x, y)
                close, wide = [], []
                for off, group in ((1, close), (2, wide)):
                    group.append(jnp.where(lane >= off, pltpu.roll(centre, off, 1), 0.0))
                    group.append(jnp.where(lane < cz - off, pltpu.roll(centre, cz - off, 1), 0.0))
                    for sign in (off, -off):
                        if 0 <= x + sign < cx:
                            group.append(own(c, x + sign, y))
                        if 0 <= y + sign < cy:
                            group.append(own(c, x, y + sign))
                weight = mass_ref[pl.ds(x * cy + y, 1), :] + 7.5
                value = (
                    weight * centre + near * functools.reduce(jnp.add, close) + far * functools.reduce(jnp.add, wide)
                )
                where = lanes((c * cx + x) * cy + y)
                image[:, where] = value
                put(qb, 0, K, where, value)
        inside = inside + against_field(c)
        advance()
    spread_mid_r = dot(four_lanes(rhs_r.T), fb[...])
    send_down(range(1))

    def arrived(c, which):
        there, piece = (
            (sub > 0, up.at[c]), (sub < n_sub - 1, down.at[c]),
            (inner > 0, left.at[:, lanes(c * side, side)]), (inner < n_inner - 1, right.at[:, lanes(c * side, side)]),
        )[which]

        @pl.when(there)
        def _():
            wait_for(piece, recv_sem.at[which, c])

    def outside(c, x, y, below):
        terms = []
        above, under = up.at[c].reshape(K * edge, cz), down.at[c].reshape(K * edge, cz)
        for off, weight in ((1, near), (2, far)):
            if below and x - off < 0:
                terms.append(weight * above[pl.ds((x - off + WIDTH) * cy + y, K, stride=edge), :])
            if below and y - off < 0:
                terms.append(weight * left[:, lanes((c * cx + x) * WIDTH + y - off + WIDTH)])
            if not below and x + off >= cx:
                terms.append(weight * under[pl.ds((x + off - cx) * cy + y, K, stride=edge), :])
            if not below and y + off >= cy:
                terms.append(weight * right[:, lanes((c * cx + x) * WIDTH + y + off - cy)])
        return functools.reduce(jnp.add, terms) if terms else None

    between = jnp.zeros((2 * K, 2 * K), F32)
    for c in range(comps):
        arrived(c, 2)
        arrived(c, 0)
        for x in range(cx):
            for y in range(cy):
                where = lanes((c * cx + x) * cy + y)
                value = outside(c, x, y, True)
                if value is None:
                    qb[:, where] = jnp.zeros((2 * K, cz), BF16)
                else:
                    image[:, where] = image[:, where] + value
                    put(qb, 0, K, where, value)
        between = between + against_field(c)
    (inside,), (between,) = pairs(inside), pairs(between)
    gram_part = inside + between + between.T
    spread(
        spread_mid_r, jnp.concatenate([gram_part, proj.T, jnp.zeros((K, cz - 2 * K), F32)], axis=1), early,
    )
    advance(last=True)
    for d, b in list(enumerate(inners))[1:]:
        remote(early.at[pl.ds(b * n_sub, n_sub), travel], early_a.at[d, :, travel], sum_sem.at[0], sum_sem.at[1],
               {inner_axis: b}).start()
    send_down(range(1, comps))

    def inner_sum():
        wait_for(early_a.at[pl.ds(1, n_inner - 1), :, travel], sum_sem.at[1])
        for s in range(n_sub):
            for rows in (pl.ds(0, TILE), pl.ds(TILE, 1)):
                value = early[inner * n_sub + s, rows]
                for d in range(1, n_inner):
                    value = value + early_a[d, s, rows]
                held[s, rows] = value
        for d, a in list(enumerate(subs))[1:]:
            remote(held.at[a, travel], early_b.at[d, travel], sum_sem.at[2], sum_sem.at[3], {sub_axis: a}).start()

    def sub_sum():
        wait_for(early_b.at[pl.ds(1, n_sub - 1), travel], sum_sem.at[3])
        for rows in (pl.ds(0, TILE), pl.ds(TILE, 1)):
            value = held[sub, rows]
            for d in range(1, n_sub):
                value = value + early_b[d, rows]
            early_full[me, rows] = value
        for a in subs[1:]:
            remote(early_full.at[me, travel], early_full.at[me, travel], sum_sem.at[4], sum_sem.at[5],
                   {sub_axis: a}).start()

    def spread_inner():
        wait_for(early_b.at[pl.ds(1, n_sub - 1), travel], sum_sem.at[5])
        block = pl.ds(inner * n_sub, n_sub)
        for b in inners[1:]:
            remote(early_full.at[block, travel], early_full.at[block, travel], sum_sem.at[6], sum_sem.at[7],
                   {inner_axis: b}).start()

    between_chunks = [inner_sum, sub_sum]
    total = jnp.zeros((6 * K, 2 * K), F32)
    for c in range(comps):
        arrived(c, 3)
        arrived(c, 1)
        for x in range(cx):
            for y in range(cy):
                where = lanes((c * cx + x) * cy + y)
                value = outside(c, x, y, False)
                kept = image[:, where]
                put(qb, 0, K, where, kept if value is None else kept + value)
        turned = lined(qb, c)
        for i in range(nodes):
            put(xb, LQ, 2 * K, lanes(c * nodes + i), turned[i * K : (i + 1) * K])
        part = pl.ds(c * chunk, chunk)
        total = total + dot_t(xb[pl.ds(0, 6 * K), part], qb[:, part])
        if c < comps - 1 and between_chunks:
            between_chunks.pop(0)()

    total = total[:, :K] + total[:, K:]
    lined_r_part, lined_q_part = (total[i : i + K] + total[i + 2 * K : i + 3 * K] for i in (0, K))
    rhs_q = total[4 * K : 5 * K] + total[5 * K :]
    spread(
        dot(four_lanes(rhs_q.T), fb[...]),
        jnp.concatenate([lined_r_part, lined_q_part, jnp.zeros((K, cz - 2 * K), F32)], axis=1),
        parts,
    )
    peers = [
        (j * n_sub + i, b * n_sub + a, {sub_axis: a, inner_axis: b})
        for i, a in enumerate(subs) for j, b in enumerate(inners) if i or j
    ]
    for d, peer, target in peers:
        remote(parts.at[peer, travel], landed.at[d, travel], sum_sem.at[8], sum_sem.at[9], target).start()
    for step in between_chunks:
        step()
    spread_inner()

    wait_for(landed.at[pl.ds(1, n - 1), travel], sum_sem.at[9])
    for rows in (pl.ds(0, TILE), pl.ds(TILE, 1)):
        mine = parts[me, rows]
        for d in range(1, n):
            mine = mine + landed[d, rows]
        full[me, rows] = mine
    for _, _, target in peers:
        remote(full.at[me, travel], full.at[me, travel], sum_sem.at[10], sum_sem.at[11], target).start()

    wait_for(early_full.at[pl.ds(0, n - n_sub), travel], sum_sem.at[7])
    mid_r, sums_r = collect(early_full)
    inv = inverse_cholesky(sums_r[:, :K])

    def solve_t(rhs_t):
        return dot(dot_t(rhs_t, inv, EXACT), inv, EXACT)

    alpha_t = solve_t(sums_r[:, K : 2 * K])
    ah, al = split(alpha_t)
    none = jnp.zeros((K, K), BF16)
    unit = (lax.broadcasted_iota(jnp.int32, (K, K), 0) == lax.broadcasted_iota(jnp.int32, (K, K), 1)).astype(BF16)

    def table(rows):
        return jnp.concatenate([jnp.concatenate(row, axis=1) for row in rows], axis=0)

    on_lines = table([[unit, -ah, unit, -ah], [none, -al, none, none]])
    on_pair = table([[ah, ah], [al, none]])
    s_flat, r_flat = (nat.reshape(K * M, cz) for nat in (s_nat, r_nat))
    outs = [ref.reshape(K * M, cz) for ref in (s_out, r_out, d_out)]
    for c in range(comps):
        part = pl.ds(c * chunk, chunk)
        image[:, part] = fold(dot(on_lines, xb[pl.ds(0, 4 * K), part]), K)
        moved = fold(dot(on_pair, xb[pl.ds(PP, 2 * K), part]), K)
        drop = fold(dot(on_pair, qb[:, part]), K)
        for i in range(nodes):
            rows = pl.ds(c * nodes + i, K, stride=M)
            cut = slice(i * cz, (i + 1) * cz)
            outs[0][rows, :] = s_flat[rows, :] + moved[:, cut]
            outs[1][rows, :] = r_flat[rows, :] - drop[:, cut]

    wait_for(landed.at[pl.ds(1, n - 1), travel], sum_sem.at[11])
    mid_q, sums_q = collect(full)
    mid_new = mid_r - dot(four_lanes(alpha_t), four_rows(mid_q))
    last = fold(dot_t(
        jnp.concatenate(split(mid_new), axis=0),
        jnp.concatenate([*split(mid_q), fb[pl.ds(0, K), :], fb[pl.ds(2 * K, K), :]], axis=0),
    ), K)
    crossed, coarse_t = last[:, :K] + last[:, K : 2 * K], last[:, 2 * K : 3 * K] + last[:, 3 * K :]
    cross_t = sums_q[:, :K] - dot(alpha_t, sums_q[:, K : 2 * K], EXACT) + crossed
    (bh, bl), (ch, cl) = split(-solve_t(cross_t)), split(coarse_t)
    on_fields = table([[ch, ch, bh, bh], [cl, none, bl, none]])
    for c in range(comps):
        part = pl.ds(c * chunk, chunk)
        turned = image[:, part] + fold(dot(on_fields, xb[pl.ds(B, 4 * K), part]), K)
        for i in range(nodes):
            outs[2][pl.ds(c * nodes + i, K, stride=M), :] = turned[:, i * cz : (i + 1) * cz]

    for which, there, buffer in (
        (0, sub < n_sub - 1, up), (1, sub > 0, down), (2, inner < n_inner - 1, left), (3, inner > 0, right),
    ):
        @pl.when(there)
        def _(which=which, buffer=buffer):
            for c in range(comps):
                piece = buffer.at[c] if which < 2 else buffer.at[:, lanes(c * side, side)]
                wait_for(piece, send_sem.at[which, c])
    for i, count in ((0, n - n_sub), (2, n_sub - 1), (4, n_sub - 1), (6, n - n_sub), (8, n - 1), (10, n - 1)):
        wait_for(full.at[pl.ds(0, count), travel], sum_sem.at[i])


def write_kernel(*refs):
    count = len(refs) // 2
    sources, targets, sem = refs[:count], refs[count : 2 * count], refs[-1]
    copies = [pltpu.make_async_copy(a, b, sem.at[i]) for i, (a, b) in enumerate(zip(sources, targets))]
    for copy in copies:
        copy.start()
    for copy in copies:
        copy.wait()


def on_device(axes, sizes, solution, residual, direction, mass, coarse_basis, line_inverse, coarse_factor):
    K, comps, cx, cy, cz = direction.shape
    n = sizes[0] * sizes[1]
    NC = coarse_factor.shape[1]
    nodes, M = cx * cy, comps * cx * cy
    assert K * NC == n * TILE * cz and K <= n and 4 * K <= cz and WIDTH * cy == TILE
    flat = (K, comps, nodes, cz)
    vmem = pl.BlockSpec(memory_space=pltpu.VMEM)
    hbm = pl.BlockSpec(memory_space=pltpu.HBM)
    dma = pltpu.SemaphoreType.DMA
    natural = pltpu.VMEM(flat, F32)
    wide = pltpu.VMEM((K, M * cz), F32)
    across = pltpu.VMEM((comps, K, WIDTH * cy, cz), F32)
    beside = pltpu.VMEM((K, comps * cx * WIDTH * cz), F32)
    slots, line = (pltpu.VMEM((count, SLOT, cz), F32) for count in (n, sizes[0]))
    inputs = (
        direction.reshape(flat), residual.reshape(flat), solution.reshape(flat), coarse_basis.reshape(flat),
        mass.reshape(nodes, cz), line_inverse.reshape(cz, cz), coarse_factor,
    )
    outs = pl.pallas_call(
        functools.partial(step_kernel, axes, sizes),
        out_shape=[jax.ShapeDtypeStruct(flat, F32)] * 3,
        in_specs=[hbm] * 7,
        out_specs=[vmem] * 3,
        scratch_shapes=[
            natural, natural, natural, natural, wide, wide,
            pltpu.VMEM((8 * K, M * cz), BF16), pltpu.VMEM((2 * K, M * cz), BF16), pltpu.VMEM((2 * K, M * cz), BF16),
            pltpu.VMEM((4 * K, NC), BF16),
            across, across, beside, beside,
            slots, pltpu.VMEM((sizes[1], sizes[0], SLOT, cz), F32), line, line, slots, slots, slots, slots,
            pltpu.VMEM((nodes, cz), F32), pltpu.VMEM((cz, cz), F32), pltpu.VMEM(coarse_factor.shape, F32),
            dma((7,)), dma((4, comps)), dma((4, comps)), dma((12,)),
            pltpu.SemaphoreType.REGULAR((2, 8)),
        ],
        compiler_params=pltpu.CompilerParams(collective_id=0, has_side_effects=True, vmem_limit_bytes=48 << 20),
    )(*[pltpu.with_memory_space_constraint(array, pltpu.HBM) for array in inputs])
    outs = pl.pallas_call(
        write_kernel,
        out_shape=[jax.ShapeDtypeStruct(flat, F32)] * 3,
        in_specs=[vmem] * 3,
        out_specs=[hbm] * 3,
        scratch_shapes=[dma((3,))],
        compiler_params=pltpu.CompilerParams(vmem_limit_bytes=1 << 20),
    )(*outs)
    return tuple(out.reshape(direction.shape) for out in outs)


def solution(mesh):
    axes = tuple(mesh.axis_names)
    sizes = tuple(mesh.shape[a] for a in axes)
    sub, inner = axes
    field = P(None, None, sub, inner, None)
    return jax.shard_map(
        functools.partial(on_device, axes, sizes),
        mesh=mesh,
        in_specs=(field, field, field, P(sub, inner, None), field, P(sub, inner, None, None), P((sub, inner), None)),
        out_specs=(field, field, field),
        check_vma=False,
    )
```

```python
import functools

import jax
import jax.numpy as jnp
from jax import lax
from jax.experimental import pallas as pl
from jax.experimental.pallas import tpu as pltpu
from jax.sharding import PartitionSpec as P

MESH = pl.DeviceIdType.MESH
EXACT = lax.Precision.HIGHEST
F32 = jnp.float32
BF16 = jnp.bfloat16
WIDTH = 2
TILE = 8
SLOT = 2 * TILE
USED = TILE + 1


def dot(a, b, precision=None):
    return lax.dot_general(a, b, (((1,), (0,)), ((), ())), precision=precision, preferred_element_type=F32)


def dot_t(a, b, precision=None):
    return lax.dot_general(a, b, (((1,), (1,)), ((), ())), precision=precision, preferred_element_type=F32)


def split(x):
    high = x.astype(BF16)
    return high, (x - high.astype(F32)).astype(BF16)


def fold(x, rows):
    return x[:rows] + x[rows:]


def inverse_cholesky(gram):
    size = gram.shape[0]
    rows = lax.broadcasted_iota(jnp.int32, (size, size), 0)
    columns = lax.broadcasted_iota(jnp.int32, (size, size), 1)
    work = jnp.concatenate([gram, (rows == columns).astype(F32)], axis=1)
    below = lax.broadcasted_iota(jnp.int32, work.shape, 0)
    for j in range(size):
        scale = lax.rsqrt(work[j : j + 1, j : j + 1])
        row = work[j : j + 1, :] * scale
        column = work[:, j : j + 1] * scale
        work = jnp.where(below > j, work - column * row, jnp.where(below == j, row, work))
    return work[:, size:]


def reaches(sizes):
    found = [1]
    while found[-1] < max(sizes) - 1:
        found.append(2 * found[-1])
    return [reach for reach in found if reach < max(sizes) - 1]


def step_kernel(
    axes, sizes,
    p_hbm, r_hbm, s_hbm, b_hbm, mass_hbm, line_hbm, factor_hbm,
    s_out, r_out, local, xf, table_out,
    p_nat, r_nat, s_nat, b_nat, field, image, xl, qb, rb, fb, up, down, left, right,
    early, early_a, held, early_b, early_full, rows_out, rows_in, rows_all, parts, landed, full,
    mass_ref, line_ref, factor_ref,
    load_sem, send_sem, sub_sem, side_sem, sum_sem, ready_sem,
):
    (sub_axis, inner_axis), (n_sub, n_inner) = axes, sizes
    n = n_sub * n_inner
    K, comps, nodes, cz = p_hbm.shape
    cy = TILE // WIDTH
    cx = nodes // cy
    M = comps * nodes
    chunk = nodes * cz
    NC = factor_hbm.shape[1]
    per_row = NC // cz
    edge = WIDTH * cy
    side = cx * WIDTH
    sub, inner = lax.axis_index(sub_axis), lax.axis_index(inner_axis)
    me = inner * n_sub + sub
    LR, LQ, B, PP = 0, K, 0, 2 * K
    travel = pl.ds(0, USED)
    tile, one = pl.ds(0, TILE), pl.ds(0, 1)

    def around(index, count):
        return [index] + [jnp.where(index + d < count, index + d, index + d - count) for d in range(1, count)]

    subs, inners = around(sub, n_sub), around(inner, n_inner)
    lines = ((sub_axis, sub, n_sub), (inner_axis, inner, n_inner))

    def greet(sem_of, reach):
        for which, (axis, index, count) in enumerate(lines):
            if reach < count:
                @pl.when(index + reach < count)
                def _():
                    pl.semaphore_signal(sem_of(which), inc=1, device_id={axis: index + reach}, device_id_type=MESH)

                @pl.when(index >= reach)
                def _():
                    pl.semaphore_signal(sem_of(which), inc=1, device_id={axis: index - reach}, device_id_type=MESH)

    def heard(index, count, reach):
        return (index + reach < count).astype(jnp.int32) + (index >= reach).astype(jnp.int32)

    barrier = pltpu.get_barrier_semaphore()
    greet(lambda which: barrier, 1)
    loads = []
    for i, (src, dst) in enumerate((
        (p_hbm, p_nat), (r_hbm, r_nat), (line_hbm, line_ref), (b_hbm, b_nat), (mass_hbm, mass_ref),
        (factor_hbm, factor_ref), (s_hbm, s_nat),
    )):
        loads.append(pltpu.make_async_copy(src, dst, load_sem.at[i]))
        loads[-1].start()
    pl.semaphore_wait(barrier, heard(sub, n_sub, 1) + heard(inner, n_inner, 1))

    rounds = reaches(sizes)

    def listen(step):
        for which, (axis, index, count) in enumerate(lines):
            if rounds[step] < count - 1:
                pl.semaphore_wait(ready_sem.at[which, step], heard(index, count, rounds[step]))

    def say(step):
        for which, (axis, index, count) in enumerate(lines):
            if rounds[step] < count - 1:
                @pl.when(index + rounds[step] < count)
                def _():
                    pl.semaphore_signal(ready_sem.at[which, step], inc=1, device_id={axis: index + rounds[step]},
                                        device_id_type=MESH)

                @pl.when(index >= rounds[step])
                def _():
                    pl.semaphore_signal(ready_sem.at[which, step], inc=1, device_id={axis: index - rounds[step]},
                                        device_id_type=MESH)

    spoken = [0]

    def advance(last=False):
        while spoken[0] < len(rounds):
            listen(spoken[0])
            spoken[0] += 1
            if spoken[0] < len(rounds):
                say(spoken[0])
            if not last:
                break

    def remote(src, dst, ssem, rsem, target):
        return pltpu.make_async_remote_copy(
            src_ref=src, dst_ref=dst, send_sem=ssem, recv_sem=rsem, device_id=target, device_id_type=MESH
        )

    def wait_for(ref, sem):
        pltpu.make_async_copy(ref, ref, sem).wait()

    def lanes(m, count=1):
        return pl.ds(m * cz, count * cz)

    def tile_rows(nat, m):
        return nat.reshape(K * M, cz)[pl.ds(m, K, stride=M), :]

    def put(ref, row, distance, where, value):
        high, low = split(value)
        ref[pl.ds(row, K), where] = high
        ref[pl.ds(row + distance, K), where] = low

    @pl.when(sub < n_sub - 1)
    def _():
        for c in range(comps):
            remote(p_hbm.at[:, c, pl.ds(nodes - edge, edge)], up.at[c], send_sem.at[0], sub_sem.at[0, c],
                   {sub_axis: sub + 1}).start()

    def send_down(some):
        @pl.when(sub > 0)
        def _():
            for c in some:
                remote(p_hbm.at[:, c, pl.ds(0, edge)], down.at[c], send_sem.at[1], sub_sem.at[1, c],
                       {sub_axis: sub - 1}).start()

    if rounds:
        say(0)
    loads[0].wait()
    for m in range(M):
        value = tile_rows(p_nat, m)
        field[:, lanes(m)] = value
        put(xf, PP, K, lanes(m), value)

    @pl.when(inner < n_inner - 1)
    def _():
        for c in range(comps):
            for x in range(cx):
                remote(field.at[:, lanes((c * cx + x) * cy + cy - WIDTH, WIDTH)],
                       left.at[:, lanes((c * cx + x) * WIDTH, WIDTH)],
                       send_sem.at[2], side_sem.at[0], {inner_axis: inner + 1}).start()

    @pl.when(inner > 0)
    def _():
        for c in range(comps):
            for x in range(cx):
                remote(field.at[:, lanes((c * cx + x) * cy, WIDTH)],
                       right.at[:, lanes((c * cx + x) * WIDTH, WIDTH)],
                       send_sem.at[3], side_sem.at[1], {inner_axis: inner - 1}).start()

    for buffer, alone in (
        (up, sub == 0), (down, sub == n_sub - 1), (left, inner == 0), (right, inner == n_inner - 1),
    ):
        @pl.when(alone)
        def _(buffer=buffer):
            buffer[...] = jnp.zeros_like(buffer)

    for load in loads[1:]:
        load.wait()
    advance()
    for m in range(M):
        put(rb, 0, K, lanes(m), tile_rows(r_nat, m))
        put(xf, B, K, lanes(m), tile_rows(b_nat, m))
    for i, half in enumerate(split(factor_ref[...])):
        fb[pl.ds(i * K, K), :] = half

    def through_factor(rhs_t):
        both = jnp.concatenate(split(rhs_t), axis=0)
        return fold(dot(both, fb[pl.ds(0, K), :]) + dot(both, fb[pl.ds(K, K), :]), K)
    advance()

    def pairs(x):
        x = x[:, :K] + x[:, K:]
        return [x[i : i + K] + x[i + K : i + 2 * K] for i in range(0, x.shape[0], 2 * K)]

    with_r = jnp.zeros((4 * K, 2 * K), F32)
    for c in range(comps):
        part = pl.ds(c * chunk, chunk)
        with_r = with_r + dot_t(xf[:, part], rb[:, part])
    rhs_r, proj = pairs(with_r)

    def spread(mid, slots):
        for t in range(n):
            a, b = t // per_row, t % per_row
            slots[t, tile, :] = mid[a * TILE : (a + 1) * TILE, b * cz : (b + 1) * cz]

    def collect(whole):
        return jnp.concatenate(
            [
                jnp.concatenate([whole[a * per_row + b, tile] for b in range(per_row)], axis=1)
                for a in range(K // TILE)
            ],
            axis=0,
        )

    def row_view(slots, at):
        depth = slots.shape[1]
        return slots.reshape(n * depth, cz).at[pl.ds(at, K, stride=depth), :]

    def padded(*blocks):
        return jnp.concatenate([*blocks, jnp.zeros((K, cz - K * len(blocks)), F32)], axis=1)

    line_high, line_low = split(line_ref[...])
    line_both = jnp.concatenate([line_high, line_high], axis=1)

    def put_lined(row, source, start, count):
        high = jnp.concatenate([source[pl.ds(0, K), lanes(start + i)] for i in range(count)], axis=0)
        low = jnp.concatenate([source[pl.ds(K, K), lanes(start + i)] for i in range(count)], axis=0)
        turned = dot_t(jnp.concatenate([high, low], axis=1), line_both) + dot_t(high, line_low)
        for i in range(count):
            put(xl, row, 2 * K, lanes(start + i), turned[i * K : (i + 1) * K])

    lane = lax.broadcasted_iota(jnp.int32, (K, cz), 1)
    near, far = -4.0 / 3.0, 1.0 / 12.0

    def own(c, x, y):
        return field[:, lanes((c * cx + x) * cy + y)]

    def against_field(c):
        part = pl.ds(c * chunk, chunk)
        return dot_t(xf[pl.ds(PP, 2 * K), part], qb[:, part])

    inside = jnp.zeros((2 * K, 2 * K), F32)
    for c in range(comps):
        put_lined(LR, rb, c * nodes, nodes)
        for x in range(cx):
            for y in range(cy):
                centre = own(c, x, y)
                close, wide = [], []
                for off, group in ((1, close), (2, wide)):
                    group.append(jnp.where(lane >= off, pltpu.roll(centre, off, 1), 0.0))
                    group.append(jnp.where(lane < cz - off, pltpu.roll(centre, cz - off, 1), 0.0))
                    for sign in (off, -off):
                        if 0 <= x + sign < cx:
                            group.append(own(c, x + sign, y))
                        if 0 <= y + sign < cy:
                            group.append(own(c, x, y + sign))
                weight = mass_ref[pl.ds(x * cy + y, 1), :] + 7.5
                value = (
                    weight * centre + near * functools.reduce(jnp.add, close) + far * functools.reduce(jnp.add, wide)
                )
                where = lanes((c * cx + x) * cy + y)
                image[:, where] = value
                put(qb, 0, K, where, value)
        inside = inside + against_field(c)
        advance()
    advance(last=True)
    spread(through_factor(rhs_r.T), early)
    for d, b in list(enumerate(inners))[1:]:
        remote(early.at[pl.ds(b * n_sub, n_sub)], early_a.at[d], sum_sem.at[0], sum_sem.at[1], {inner_axis: b}).start()

    @pl.when(sub < n_sub - 1)
    def _():
        wait_for(up, send_sem.at[0])
    send_down(range(1))

    def arrived(there, buffer, sem):
        @pl.when(there)
        def _():
            wait_for(buffer, sem)

    def outside(c, x, y, below):
        terms = []
        above, under = up.at[c].reshape(K * edge, cz), down.at[c].reshape(K * edge, cz)
        for off, weight in ((1, near), (2, far)):
            if below and x - off < 0:
                terms.append(weight * above[pl.ds((x - off + WIDTH) * cy + y, K, stride=edge), :])
            if below and y - off < 0:
                terms.append(weight * left[:, lanes((c * cx + x) * WIDTH + y - off + WIDTH)])
            if not below and x + off >= cx:
                terms.append(weight * under[pl.ds((x + off - cx) * cy + y, K, stride=edge), :])
            if not below and y + off >= cy:
                terms.append(weight * right[:, lanes((c * cx + x) * WIDTH + y + off - cy)])
        return functools.reduce(jnp.add, terms) if terms else None

    def inner_sum():
        wait_for(early_a.at[pl.ds(1, n_inner - 1)], sum_sem.at[1])
        for s in range(n_sub):
            value = early[inner * n_sub + s]
            for d in range(1, n_inner):
                value = value + early_a[d, s]
            held[s] = value
        for d, a in list(enumerate(subs))[1:]:
            remote(held.at[a], early_b.at[d], sum_sem.at[2], sum_sem.at[3], {sub_axis: a}).start()

    def sub_sum():
        wait_for(early_b.at[pl.ds(1, n_sub - 1)], sum_sem.at[3])
        value = held[sub]
        for d in range(1, n_sub):
            value = value + early_b[d]
        early_full[me] = value
        for a in subs[1:]:
            remote(early_full.at[me], early_full.at[me], sum_sem.at[4], sum_sem.at[5], {sub_axis: a}).start()

    def spread_inner():
        wait_for(early_b.at[pl.ds(1, n_sub - 1)], sum_sem.at[5])
        block = pl.ds(inner * n_sub, n_sub)
        for b in inners[1:]:
            remote(early_full.at[block], early_full.at[block], sum_sem.at[6], sum_sem.at[7], {inner_axis: b}).start()

    between = jnp.zeros((2 * K, 2 * K), F32)
    arrived(inner > 0, left, side_sem.at[0])
    for c in range(comps):
        arrived(sub > 0, up.at[c], sub_sem.at[0, c])
        for x in range(cx):
            for y in range(cy):
                where = lanes((c * cx + x) * cy + y)
                value = outside(c, x, y, True)
                if value is None:
                    qb[:, where] = jnp.zeros((2 * K, cz), BF16)
                else:
                    image[:, where] = image[:, where] + value
                    put(qb, 0, K, where, value)
        between = between + against_field(c)
    (inside,), (between,) = pairs(inside), pairs(between)
    gram_part = inside + between + between.T
    row_view(rows_out, 0)[...] = padded(gram_part, proj.T)
    peers = [
        (j * n_sub + i, b * n_sub + a, {sub_axis: a, inner_axis: b})
        for i, a in enumerate(subs) for j, b in enumerate(inners) if i or j
    ]
    inner_sum()
    for d, peer, target in peers:
        remote(rows_out.at[peer, one], rows_in.at[d, one], sum_sem.at[12], sum_sem.at[13], target).start()
    send_down(range(1, comps))

    def row_sum():
        wait_for(rows_in.at[pl.ds(1, n - 1), one], sum_sem.at[13])
        value = rows_out[me, one]
        for d in range(1, n):
            value = value + rows_in[d, one]
        rows_all[me, one] = value
        for _, _, target in peers:
            remote(rows_all.at[me, one], rows_all.at[me, one], sum_sem.at[14], sum_sem.at[15], target).start()

    def image_terms(c, rows):
        for x in rows:
            for y in range(cy):
                where = lanes((c * cx + x) * cy + y)
                value = outside(c, x, y, False)
                kept = image[:, where]
                put(qb, 0, K, where, kept if value is None else kept + value)
        start, count = c * nodes + rows[0] * cy, len(rows) * cy
        put_lined(LQ, qb, start, count)
        part = lanes(start, count)
        return dot_t(xl[:, part], qb[:, part]), dot_t(qb[:, part], xf[pl.ds(B, 2 * K), part])

    total, rhs_q = jnp.zeros((4 * K, 2 * K), F32), jnp.zeros((2 * K, 2 * K), F32)
    arrived(inner < n_inner - 1, right, side_sem.at[1])
    for c in range(comps):
        more, more_rhs = image_terms(c, range(cx - WIDTH))
        total, rhs_q = total + more, rhs_q + more_rhs
    for c in range(comps):
        arrived(sub < n_sub - 1, down.at[c], sub_sem.at[1, c])
        more, more_rhs = image_terms(c, range(cx - WIDTH, cx))
        total, rhs_q = total + more, rhs_q + more_rhs
        if c == comps - 2:
            sub_sum()
            row_sum()

    total = total[:, :K] + total[:, K:]
    lined_r_part, lined_q_part = (total[i : i + K] + total[i + 2 * K : i + 3 * K] for i in (0, K))
    rhs_q = fold(rhs_q, K)
    spread(through_factor(rhs_q[:, :K] + rhs_q[:, K:]), parts)
    row_view(parts, TILE)[...] = padded(lined_r_part, lined_q_part)
    for d, peer, target in peers:
        remote(parts.at[peer, travel], landed.at[d, travel], sum_sem.at[8], sum_sem.at[9], target).start()

    wait_for(rows_all.at[pl.ds(0, n - 1), one], sum_sem.at[15])
    sums_r = row_view(rows_all, 0)[...]
    inv = inverse_cholesky(sums_r[:, :K])


    wait_for(landed.at[pl.ds(1, n - 1), travel], sum_sem.at[9])
    for rows in (tile, pl.ds(TILE, 1)):
        value = parts[me, rows]
        for d in range(1, n):
            value = value + landed[d, rows]
        full[me, rows] = value
    for _, _, target in peers:
        remote(full.at[me, travel], full.at[me, travel], sum_sem.at[10], sum_sem.at[11], target).start()
    spread_inner()

    alpha_t = dot(dot_t(sums_r[:, K : 2 * K], inv, EXACT), inv, EXACT)
    gram_inverse = dot(inv.T, inv, EXACT)
    ah, al = split(alpha_t)
    none = jnp.zeros((K, K), BF16)
    unit = (lax.broadcasted_iota(jnp.int32, (K, K), 0) == lax.broadcasted_iota(jnp.int32, (K, K), 1)).astype(BF16)

    def table(rows):
        return jnp.concatenate([jnp.concatenate(row, axis=1) for row in rows], axis=0)

    on_lines = table([[unit, -ah, unit, -ah], [none, -al, none, none]])
    on_pair = table([[ah, ah], [al, none]])
    s_flat, r_flat = (nat.reshape(K * M, cz) for nat in (s_nat, r_nat))
    outs = [ref.reshape(K * M, cz) for ref in (s_out, r_out)]
    for c in range(comps):
        part = pl.ds(c * chunk, chunk)
        local[:, part] = fold(dot(on_lines, xl[:, part]), K)
        moved = fold(dot(on_pair, xf[pl.ds(PP, 2 * K), part]), K)
        drop = fold(dot(on_pair, qb[:, part]), K)
        for i in range(nodes):
            rows = pl.ds(c * nodes + i, K, stride=M)
            cut = slice(i * cz, (i + 1) * cz)
            outs[0][rows, :] = s_flat[rows, :] + moved[:, cut]
            outs[1][rows, :] = r_flat[rows, :] - drop[:, cut]

    wait_for(early_full.at[pl.ds(0, n - n_sub)], sum_sem.at[7])
    mid_r = jnp.concatenate(split(collect(early_full)), axis=0)

    wait_for(full.at[pl.ds(0, n - 1), travel], sum_sem.at[11])
    mid_q, sums_q = jnp.concatenate(split(collect(full)), axis=0), row_view(full, TILE)[...]
    meet = dot_t(jnp.concatenate([mid_q, mid_r], axis=0), jnp.concatenate([mid_q, fb[...]], axis=0))
    from_q, from_r = fold(meet[: 2 * K], K), fold(meet[2 * K :], K)
    taken = dot(alpha_t, jnp.concatenate(
        [from_q[:, :K] + from_q[:, K : 2 * K] + sums_q[:, K : 2 * K], from_q[:, 2 * K : 3 * K] + from_q[:, 3 * K :]], axis=1,
    ), EXACT)
    cross_t = sums_q[:, :K] + from_r[:, :K] + from_r[:, K : 2 * K] - taken[:, :K]
    coarse_t = from_r[:, 2 * K : 3 * K] + from_r[:, 3 * K :] - taken[:, K:]
    (bh, bl), (ch, cl) = split(-dot(cross_t, gram_inverse, EXACT)), split(coarse_t)
    table_out[...] = table([[ch, ch, bh, bh], [cl, none, bl, none]])

    arrived(sub > 0, down, send_sem.at[1])
    arrived(inner < n_inner - 1, left, send_sem.at[2])
    arrived(inner > 0, right, send_sem.at[3])
    for i, count in ((0, n - n_sub), (2, n_sub - 1), (4, n_sub - 1), (6, n - n_sub)):
        wait_for(early_full.at[pl.ds(0, count)], sum_sem.at[i])
    for i in (12, 14):
        wait_for(rows_all.at[pl.ds(0, n - 1), one], sum_sem.at[i])
    for i in (8, 10):
        wait_for(full.at[pl.ds(0, n - 1), travel], sum_sem.at[i])


def write_kernel(s_in, r_in, local, xf, table, s_hbm, r_hbm, d_hbm, d_nat, sem):
    K, comps, nodes, cz = s_in.shape
    M = comps * nodes
    copies = [pltpu.make_async_copy(s_in, s_hbm, sem.at[0]), pltpu.make_async_copy(r_in, r_hbm, sem.at[1])]
    for copy in copies:
        copy.start()
    mix = table[...]
    flat = d_nat.reshape(K * M, cz)
    for c in range(comps):
        part = pl.ds(c * nodes * cz, nodes * cz)
        turned = local[:, part] + fold(dot(mix, xf[:, part]), K)
        for i in range(nodes):
            flat[pl.ds(c * nodes + i, K, stride=M), :] = turned[:, i * cz : (i + 1) * cz]
        copies.append(pltpu.make_async_copy(d_nat.at[:, c], d_hbm.at[:, c], sem.at[2 + c]))
        copies[-1].start()
    for copy in copies:
        copy.wait()


def on_device(axes, sizes, solution, residual, direction, mass, coarse_basis, line_inverse, coarse_factor):
    K, comps, cx, cy, cz = direction.shape
    n = sizes[0] * sizes[1]
    NC = coarse_factor.shape[1]
    nodes, M = cx * cy, comps * cx * cy
    assert K * NC == n * TILE * cz and K <= n and 4 * K <= cz and WIDTH * cy == TILE
    flat = (K, comps, nodes, cz)
    vmem = pl.BlockSpec(memory_space=pltpu.VMEM)
    hbm = pl.BlockSpec(memory_space=pltpu.HBM)
    dma = pltpu.SemaphoreType.DMA
    natural = pltpu.VMEM(flat, F32)
    wide = pltpu.VMEM((K, M * cz), F32)
    across = pltpu.VMEM((comps, K, WIDTH * cy, cz), F32)
    beside = pltpu.VMEM((K, comps * cx * WIDTH * cz), F32)
    slots = pltpu.VMEM((n, SLOT, cz), F32)
    tiles, line = (pltpu.VMEM((count, TILE, cz), F32) for count in (n, sizes[0]))
    inputs = (
        direction.reshape(flat), residual.reshape(flat), solution.reshape(flat), coarse_basis.reshape(flat),
        mass.reshape(nodes, cz), line_inverse.reshape(cz, cz), coarse_factor,
    )
    outs = pl.pallas_call(
        functools.partial(step_kernel, axes, sizes),
        out_shape=[
            jax.ShapeDtypeStruct(flat, F32), jax.ShapeDtypeStruct(flat, F32), jax.ShapeDtypeStruct((K, M * cz), F32),
            jax.ShapeDtypeStruct((4 * K, M * cz), BF16), jax.ShapeDtypeStruct((2 * K, 4 * K), BF16),
        ],
        in_specs=[hbm] * 7,
        out_specs=[vmem] * 5,
        scratch_shapes=[
            natural, natural, natural, natural, wide, wide,
            pltpu.VMEM((4 * K, M * cz), BF16), pltpu.VMEM((2 * K, M * cz), BF16), pltpu.VMEM((2 * K, M * cz), BF16),
            pltpu.VMEM((2 * K, NC), BF16),
            across, across, beside, beside,
            tiles, pltpu.VMEM((sizes[1], sizes[0], TILE, cz), F32), line, line, tiles, tiles, tiles, tiles,
            slots, slots, slots,
            pltpu.VMEM((nodes, cz), F32), pltpu.VMEM((cz, cz), F32), pltpu.VMEM(coarse_factor.shape, F32),
            dma((7,)), dma((4,)), dma((2, comps)), dma((2,)), dma((16,)),
            pltpu.SemaphoreType.REGULAR((2, max(len(reaches(sizes)), 1))),
        ],
        compiler_params=pltpu.CompilerParams(collective_id=0, has_side_effects=True, vmem_limit_bytes=40 << 20),
    )(*[pltpu.with_memory_space_constraint(array, pltpu.HBM) for array in inputs])
    outs = pl.pallas_call(
        write_kernel,
        out_shape=[jax.ShapeDtypeStruct(flat, F32)] * 3,
        in_specs=[vmem] * 5,
        out_specs=[hbm] * 3,
        scratch_shapes=[natural, dma((2 + comps,))],
        compiler_params=pltpu.CompilerParams(vmem_limit_bytes=8 << 20),
    )(*outs)
    return tuple(out.reshape(direction.shape) for out in outs)


def solution(mesh):
    axes = tuple(mesh.axis_names)
    sizes = tuple(mesh.shape[a] for a in axes)
    sub, inner = axes
    field = P(None, None, sub, inner, None)
    return jax.shard_map(
        functools.partial(on_device, axes, sizes),
        mesh=mesh,
        in_specs=(field, field, field, P(sub, inner, None), field, P(sub, inner, None, None), P((sub, inner), None)),
        out_specs=(field, field, field),
        check_vma=False,
    )
```

```python
import functools

import jax
import jax.numpy as jnp
from jax import lax
from jax.experimental import pallas as pl
from jax.experimental.pallas import tpu as pltpu
from jax.sharding import PartitionSpec as P

MESH = pl.DeviceIdType.MESH
EXACT = lax.Precision.HIGHEST
F32 = jnp.float32
BF16 = jnp.bfloat16
WIDTH = 2
TILE = 8
SLOT = 2 * TILE
USED = TILE + 1


def dot(a, b, precision=None):
    return lax.dot_general(a, b, (((1,), (0,)), ((), ())), precision=precision, preferred_element_type=F32)


def dot_t(a, b, precision=None):
    return lax.dot_general(a, b, (((1,), (1,)), ((), ())), precision=precision, preferred_element_type=F32)


def split(x):
    high = x.astype(BF16)
    return high, (x - high.astype(F32)).astype(BF16)


def fold(x, rows):
    return x[:rows] + x[rows:]


def inverse_cholesky(gram):
    size = gram.shape[0]
    rows = lax.broadcasted_iota(jnp.int32, (size, size), 0)
    columns = lax.broadcasted_iota(jnp.int32, (size, size), 1)
    work = jnp.concatenate([gram, (rows == columns).astype(F32)], axis=1)
    below = lax.broadcasted_iota(jnp.int32, work.shape, 0)
    for j in range(size):
        scale = lax.rsqrt(work[j : j + 1, j : j + 1])
        row = work[j : j + 1, :] * scale
        column = work[:, j : j + 1] * scale
        work = jnp.where(below > j, work - column * row, jnp.where(below == j, row, work))
    return work[:, size:]


def reaches(sizes):
    found = [1]
    while found[-1] < max(sizes) - 1:
        found.append(2 * found[-1])
    return [reach for reach in found if reach < max(sizes) - 1]


def step_kernel(
    axes, sizes,
    p_hbm, r_hbm, s_hbm, b_hbm, mass_hbm, line_hbm, factor_hbm,
    s_out, r_out, local, xf, table_out,
    p_nat, r_nat, s_nat, b_nat, field, image, xl, qb, rb, fb, up, down, left, right,
    early, early_a, held, early_b, early_full, rows_out, rows_in, rows_all, parts, landed, full,
    mass_ref, line_ref, factor_ref,
    load_sem, send_sem, sub_sem, side_sem, sum_sem, ready_sem,
):
    (sub_axis, inner_axis), (n_sub, n_inner) = axes, sizes
    n = n_sub * n_inner
    K, comps, nodes, cz = p_hbm.shape
    cy = TILE // WIDTH
    cx = nodes // cy
    M = comps * nodes
    chunk = nodes * cz
    NC = factor_hbm.shape[1]
    per_row = NC // cz
    edge = WIDTH * cy
    side = cx * WIDTH
    sub, inner = lax.axis_index(sub_axis), lax.axis_index(inner_axis)
    me = inner * n_sub + sub
    LR, LQ, B, PP = 0, K, 0, 2 * K
    travel = pl.ds(0, USED)
    tile, one = pl.ds(0, TILE), pl.ds(0, 1)

    def around(index, count):
        return [index] + [jnp.where(index + d < count, index + d, index + d - count) for d in range(1, count)]

    subs, inners = around(sub, n_sub), around(inner, n_inner)
    lines = ((sub_axis, sub, n_sub), (inner_axis, inner, n_inner))

    def greet(sem_of, reach):
        for which, (axis, index, count) in enumerate(lines):
            if reach < count:
                @pl.when(index + reach < count)
                def _():
                    pl.semaphore_signal(sem_of(which), inc=1, device_id={axis: index + reach}, device_id_type=MESH)

                @pl.when(index >= reach)
                def _():
                    pl.semaphore_signal(sem_of(which), inc=1, device_id={axis: index - reach}, device_id_type=MESH)

    def heard(index, count, reach):
        return (index + reach < count).astype(jnp.int32) + (index >= reach).astype(jnp.int32)

    barrier = pltpu.get_barrier_semaphore()
    greet(lambda which: barrier, 1)
    loads = []
    for i, (src, dst) in enumerate((
        (p_hbm, p_nat), (r_hbm, r_nat), (line_hbm, line_ref), (b_hbm, b_nat), (mass_hbm, mass_ref),
        (factor_hbm, factor_ref), (s_hbm, s_nat),
    )):
        loads.append(pltpu.make_async_copy(src, dst, load_sem.at[i]))
        loads[-1].start()
    pl.semaphore_wait(barrier, heard(sub, n_sub, 1) + heard(inner, n_inner, 1))

    rounds = reaches(sizes)

    def listen(step):
        for which, (axis, index, count) in enumerate(lines):
            if rounds[step] < count - 1:
                pl.semaphore_wait(ready_sem.at[which, step], heard(index, count, rounds[step]))

    def say(step):
        for which, (axis, index, count) in enumerate(lines):
            if rounds[step] < count - 1:
                @pl.when(index + rounds[step] < count)
                def _():
                    pl.semaphore_signal(ready_sem.at[which, step], inc=1, device_id={axis: index + rounds[step]},
                                        device_id_type=MESH)

                @pl.when(index >= rounds[step])
                def _():
                    pl.semaphore_signal(ready_sem.at[which, step], inc=1, device_id={axis: index - rounds[step]},
                                        device_id_type=MESH)

    spoken = [0]

    def advance(last=False):
        while spoken[0] < len(rounds):
            listen(spoken[0])
            spoken[0] += 1
            if spoken[0] < len(rounds):
                say(spoken[0])
            if not last:
                break

    def remote(src, dst, ssem, rsem, target):
        return pltpu.make_async_remote_copy(
            src_ref=src, dst_ref=dst, send_sem=ssem, recv_sem=rsem, device_id=target, device_id_type=MESH
        )

    def wait_for(ref, sem):
        pltpu.make_async_copy(ref, ref, sem).wait()

    def lanes(m, count=1):
        return pl.ds(m * cz, count * cz)

    def tile_rows(nat, m):
        return nat.reshape(K * M, cz)[pl.ds(m, K, stride=M), :]

    def put(ref, row, distance, where, value):
        high, low = split(value)
        ref[pl.ds(row, K), where] = high
        ref[pl.ds(row + distance, K), where] = low

    @pl.when(sub < n_sub - 1)
    def _():
        for c in range(comps):
            remote(p_hbm.at[:, c, pl.ds(nodes - edge, edge)], up.at[c], send_sem.at[0], sub_sem.at[0, c],
                   {sub_axis: sub + 1}).start()

    def send_down(some):
        @pl.when(sub > 0)
        def _():
            for c in some:
                remote(p_hbm.at[:, c, pl.ds(0, edge)], down.at[c], send_sem.at[1], sub_sem.at[1, c],
                       {sub_axis: sub - 1}).start()

    if rounds:
        say(0)
    loads[0].wait()
    for m in range(M):
        value = tile_rows(p_nat, m)
        field[:, lanes(m)] = value
        put(xf, PP, K, lanes(m), value)

    @pl.when(inner < n_inner - 1)
    def _():
        for c in range(comps):
            for x in range(cx):
                remote(field.at[:, lanes((c * cx + x) * cy + cy - WIDTH, WIDTH)],
                       left.at[:, lanes((c * cx + x) * WIDTH, WIDTH)],
                       send_sem.at[2], side_sem.at[0], {inner_axis: inner + 1}).start()

    @pl.when(inner > 0)
    def _():
        for c in range(comps):
            for x in range(cx):
                remote(field.at[:, lanes((c * cx + x) * cy, WIDTH)],
                       right.at[:, lanes((c * cx + x) * WIDTH, WIDTH)],
                       send_sem.at[3], side_sem.at[1], {inner_axis: inner - 1}).start()

    for buffer, alone in (
        (up, sub == 0), (down, sub == n_sub - 1), (left, inner == 0), (right, inner == n_inner - 1),
    ):
        @pl.when(alone)
        def _(buffer=buffer):
            buffer[...] = jnp.zeros_like(buffer)

    for load in loads[1:]:
        load.wait()
    advance()
    for m in range(M):
        put(rb, 0, K, lanes(m), tile_rows(r_nat, m))
        put(xf, B, K, lanes(m), tile_rows(b_nat, m))
    for i, half in enumerate(split(factor_ref[...])):
        fb[pl.ds(i * K, K), :] = half

    def through_factor(rhs_t):
        both = jnp.concatenate(split(rhs_t), axis=0)
        return fold(dot(both, fb[pl.ds(0, K), :]) + dot(both, fb[pl.ds(K, K), :]), K)
    advance()

    def pairs(x):
        x = x[:, :K] + x[:, K:]
        return [x[i : i + K] + x[i + K : i + 2 * K] for i in range(0, x.shape[0], 2 * K)]

    with_r = jnp.zeros((4 * K, 2 * K), F32)
    for c in range(comps):
        part = pl.ds(c * chunk, chunk)
        with_r = with_r + dot_t(xf[:, part], rb[:, part])
    rhs_r, proj = pairs(with_r)

    def spread(mid, slots):
        for t in range(n):
            a, b = t // per_row, t % per_row
            slots[t, tile, :] = mid[a * TILE : (a + 1) * TILE, b * cz : (b + 1) * cz]

    def collect(whole):
        return jnp.concatenate(
            [
                jnp.concatenate([whole[a * per_row + b, tile] for b in range(per_row)], axis=1)
                for a in range(K // TILE)
            ],
            axis=0,
        )

    def row_view(slots, at):
        depth = slots.shape[1]
        return slots.reshape(n * depth, cz).at[pl.ds(at, K, stride=depth), :]

    def padded(*blocks):
        return jnp.concatenate([*blocks, jnp.zeros((K, cz - K * len(blocks)), F32)], axis=1)

    line_high, line_low = split(line_ref[...])
    line_both = jnp.concatenate([line_high, line_high], axis=1)

    def put_lined(row, source, start, count):
        high = jnp.concatenate([source[pl.ds(0, K), lanes(start + i)] for i in range(count)], axis=0)
        low = jnp.concatenate([source[pl.ds(K, K), lanes(start + i)] for i in range(count)], axis=0)
        turned = dot_t(jnp.concatenate([high, low], axis=1), line_both) + dot_t(high, line_low)
        for i in range(count):
            put(xl, row, 2 * K, lanes(start + i), turned[i * K : (i + 1) * K])

    lane = lax.broadcasted_iota(jnp.int32, (K, cz), 1)
    near, far = -4.0 / 3.0, 1.0 / 12.0

    def own(c, x, y):
        return field[:, lanes((c * cx + x) * cy + y)]

    def against_field(c):
        part = pl.ds(c * chunk, chunk)
        return dot_t(xf[pl.ds(PP, 2 * K), part], qb[:, part])

    inside = jnp.zeros((2 * K, 2 * K), F32)
    for c in range(comps):
        put_lined(LR, rb, c * nodes, nodes)
        for x in range(cx):
            for y in range(cy):
                centre = own(c, x, y)
                close, wide = [], []
                for off, group in ((1, close), (2, wide)):
                    group.append(jnp.where(lane >= off, pltpu.roll(centre, off, 1), 0.0))
                    group.append(jnp.where(lane < cz - off, pltpu.roll(centre, cz - off, 1), 0.0))
                    for sign in (off, -off):
                        if 0 <= x + sign < cx:
                            group.append(own(c, x + sign, y))
                        if 0 <= y + sign < cy:
                            group.append(own(c, x, y + sign))
                weight = mass_ref[pl.ds(x * cy + y, 1), :] + 7.5
                value = (
                    weight * centre + near * functools.reduce(jnp.add, close) + far * functools.reduce(jnp.add, wide)
                )
                where = lanes((c * cx + x) * cy + y)
                image[:, where] = value
                put(qb, 0, K, where, value)
        inside = inside + against_field(c)
        advance()
    advance(last=True)
    spread(through_factor(rhs_r.T), early)
    for d, b in list(enumerate(inners))[1:]:
        remote(early.at[pl.ds(b * n_sub, n_sub)], early_a.at[d], sum_sem.at[0], sum_sem.at[1], {inner_axis: b}).start()

    @pl.when(sub < n_sub - 1)
    def _():
        wait_for(up, send_sem.at[0])
    send_down(range(1))

    def arrived(there, buffer, sem):
        @pl.when(there)
        def _():
            wait_for(buffer, sem)

    def outside(c, x, y, below):
        terms = []
        above, under = up.at[c].reshape(K * edge, cz), down.at[c].reshape(K * edge, cz)
        for off, weight in ((1, near), (2, far)):
            if below and x - off < 0:
                terms.append(weight * above[pl.ds((x - off + WIDTH) * cy + y, K, stride=edge), :])
            if below and y - off < 0:
                terms.append(weight * left[:, lanes((c * cx + x) * WIDTH + y - off + WIDTH)])
            if not below and x + off >= cx:
                terms.append(weight * under[pl.ds((x + off - cx) * cy + y, K, stride=edge), :])
            if not below and y + off >= cy:
                terms.append(weight * right[:, lanes((c * cx + x) * WIDTH + y + off - cy)])
        return functools.reduce(jnp.add, terms) if terms else None

    def inner_sum():
        wait_for(early_a.at[pl.ds(1, n_inner - 1)], sum_sem.at[1])
        for s in range(n_sub):
            value = early[inner * n_sub + s]
            for d in range(1, n_inner):
                value = value + early_a[d, s]
            held[s] = value
        for d, a in list(enumerate(subs))[1:]:
            remote(held.at[a], early_b.at[d], sum_sem.at[2], sum_sem.at[3], {sub_axis: a}).start()

    def sub_sum():
        wait_for(early_b.at[pl.ds(1, n_sub - 1)], sum_sem.at[3])
        value = held[sub]
        for d in range(1, n_sub):
            value = value + early_b[d]
        early_full[me] = value
        for a in subs[1:]:
            remote(early_full.at[me], early_full.at[me], sum_sem.at[4], sum_sem.at[5], {sub_axis: a}).start()

    def spread_inner():
        wait_for(early_b.at[pl.ds(1, n_sub - 1)], sum_sem.at[5])
        block = pl.ds(inner * n_sub, n_sub)
        for b in inners[1:]:
            remote(early_full.at[block], early_full.at[block], sum_sem.at[6], sum_sem.at[7], {inner_axis: b}).start()

    between = jnp.zeros((2 * K, 2 * K), F32)
    arrived(inner > 0, left, side_sem.at[0])
    for c in range(comps):
        arrived(sub > 0, up.at[c], sub_sem.at[0, c])
        for x in range(cx):
            for y in range(cy):
                where = lanes((c * cx + x) * cy + y)
                value = outside(c, x, y, True)
                if value is None:
                    qb[:, where] = jnp.zeros((2 * K, cz), BF16)
                else:
                    image[:, where] = image[:, where] + value
                    put(qb, 0, K, where, value)
        between = between + against_field(c)
    (inside,), (between,) = pairs(inside), pairs(between)
    gram_part = inside + between + between.T
    row_view(rows_out, 0)[...] = padded(gram_part, proj.T)
    peers = [
        (j * n_sub + i, b * n_sub + a, {sub_axis: a, inner_axis: b})
        for i, a in enumerate(subs) for j, b in enumerate(inners) if i or j
    ]
    inner_sum()
    for d, peer, target in peers:
        remote(rows_out.at[peer, one], rows_in.at[d, one], sum_sem.at[12], sum_sem.at[13], target).start()
    send_down(range(1, comps))

    def row_sum():
        wait_for(rows_in.at[pl.ds(1, n - 1), one], sum_sem.at[13])
        value = rows_out[me, one]
        for d in range(1, n):
            value = value + rows_in[d, one]
        rows_all[me, one] = value
        for _, _, target in peers:
            remote(rows_all.at[me, one], rows_all.at[me, one], sum_sem.at[14], sum_sem.at[15], target).start()

    def image_terms(c, rows):
        for x in rows:
            for y in range(cy):
                where = lanes((c * cx + x) * cy + y)
                value = outside(c, x, y, False)
                kept = image[:, where]
                put(qb, 0, K, where, kept if value is None else kept + value)
        start, count = c * nodes + rows[0] * cy, len(rows) * cy
        put_lined(LQ, qb, start, count)
        part = lanes(start, count)
        return dot_t(xl[:, part], qb[:, part]), dot_t(qb[:, part], xf[pl.ds(B, 2 * K), part])

    total, rhs_q = jnp.zeros((4 * K, 2 * K), F32), jnp.zeros((2 * K, 2 * K), F32)
    arrived(inner < n_inner - 1, right, side_sem.at[1])
    for c in range(comps):
        more, more_rhs = image_terms(c, range(cx - WIDTH))
        total, rhs_q = total + more, rhs_q + more_rhs
    for c in range(comps):
        arrived(sub < n_sub - 1, down.at[c], sub_sem.at[1, c])
        more, more_rhs = image_terms(c, range(cx - WIDTH, cx))
        total, rhs_q = total + more, rhs_q + more_rhs
        if c == comps - 2:
            sub_sum()
            row_sum()

    total = total[:, :K] + total[:, K:]
    lined_r_part, lined_q_part = (total[i : i + K] + total[i + 2 * K : i + 3 * K] for i in (0, K))
    rhs_q = fold(rhs_q, K)
    spread(through_factor(rhs_q[:, :K] + rhs_q[:, K:]), parts)
    row_view(parts, TILE)[...] = padded(lined_r_part, lined_q_part)
    for d, peer, target in sorted(peers, key=lambda p: abs(p[0] % n_sub - n_sub // 2)):
        remote(parts.at[peer, travel], landed.at[d, travel], sum_sem.at[8], sum_sem.at[9], target).start()

    wait_for(landed.at[pl.ds(1, n - 1), travel], sum_sem.at[9])
    for rows in (tile, pl.ds(TILE, 1)):
        value = parts[me, rows]
        for d in range(1, n):
            value = value + landed[d, rows]
        full[me, rows] = value
    for _, _, target in peers:
        remote(full.at[me, travel], full.at[me, travel], sum_sem.at[10], sum_sem.at[11], target).start()
    spread_inner()

    wait_for(rows_all.at[pl.ds(0, n - 1), one], sum_sem.at[15])
    sums_r = row_view(rows_all, 0)[...]
    inv = inverse_cholesky(sums_r[:, :K])
    alpha_t = dot(dot_t(sums_r[:, K : 2 * K], inv, EXACT), inv, EXACT)
    gram_inverse = dot(inv.T, inv, EXACT)
    ah, al = split(alpha_t)
    none = jnp.zeros((K, K), BF16)
    unit = (lax.broadcasted_iota(jnp.int32, (K, K), 0) == lax.broadcasted_iota(jnp.int32, (K, K), 1)).astype(BF16)

    def table(rows):
        return jnp.concatenate([jnp.concatenate(row, axis=1) for row in rows], axis=0)

    on_lines = table([[unit, -ah, unit, -ah], [none, -al, none, none]])
    on_pair = table([[ah, ah], [al, none]])
    s_flat, r_flat = (nat.reshape(K * M, cz) for nat in (s_nat, r_nat))
    outs = [ref.reshape(K * M, cz) for ref in (s_out, r_out)]
    for c in range(comps):
        part = pl.ds(c * chunk, chunk)
        local[:, part] = fold(dot(on_lines, xl[:, part]), K)
        moved = fold(dot(on_pair, xf[pl.ds(PP, 2 * K), part]), K)
        drop = fold(dot(on_pair, qb[:, part]), K)
        for i in range(nodes):
            rows = pl.ds(c * nodes + i, K, stride=M)
            cut = slice(i * cz, (i + 1) * cz)
            outs[0][rows, :] = s_flat[rows, :] + moved[:, cut]
            outs[1][rows, :] = r_flat[rows, :] - drop[:, cut]

    wait_for(early_full.at[pl.ds(0, n - n_sub)], sum_sem.at[7])
    mid_r = jnp.concatenate(split(collect(early_full)), axis=0)

    wait_for(full.at[pl.ds(0, n - 1), travel], sum_sem.at[11])
    mid_q, sums_q = jnp.concatenate(split(collect(full)), axis=0), row_view(full, TILE)[...]
    meet = dot_t(jnp.concatenate([mid_q, mid_r], axis=0), jnp.concatenate([mid_q, fb[...]], axis=0))
    from_q, from_r = fold(meet[: 2 * K], K), fold(meet[2 * K :], K)
    taken = dot(alpha_t, jnp.concatenate(
        [from_q[:, :K] + from_q[:, K : 2 * K] + sums_q[:, K : 2 * K], from_q[:, 2 * K : 3 * K] + from_q[:, 3 * K :]], axis=1,
    ), EXACT)
    cross_t = sums_q[:, :K] + from_r[:, :K] + from_r[:, K : 2 * K] - taken[:, :K]
    coarse_t = from_r[:, 2 * K : 3 * K] + from_r[:, 3 * K :] - taken[:, K:]
    (bh, bl), (ch, cl) = split(-dot(cross_t, gram_inverse, EXACT)), split(coarse_t)
    table_out[...] = table([[ch, ch, bh, bh], [cl, none, bl, none]])

    arrived(sub > 0, down, send_sem.at[1])
    arrived(inner < n_inner - 1, left, send_sem.at[2])
    arrived(inner > 0, right, send_sem.at[3])
    for i, count in ((0, n - n_sub), (2, n_sub - 1), (4, n_sub - 1), (6, n - n_sub)):
        wait_for(early_full.at[pl.ds(0, count)], sum_sem.at[i])
    for i in (12, 14):
        wait_for(rows_all.at[pl.ds(0, n - 1), one], sum_sem.at[i])
    for i in (8, 10):
        wait_for(full.at[pl.ds(0, n - 1), travel], sum_sem.at[i])


def write_kernel(s_in, r_in, local, xf, table, s_hbm, r_hbm, d_hbm, d_nat, sem):
    K, comps, nodes, cz = s_in.shape
    M = comps * nodes
    copies = [pltpu.make_async_copy(s_in, s_hbm, sem.at[0]), pltpu.make_async_copy(r_in, r_hbm, sem.at[1])]
    for copy in copies:
        copy.start()
    mix = table[...]
    flat = d_nat.reshape(K * M, cz)
    for c in range(comps):
        part = pl.ds(c * nodes * cz, nodes * cz)
        turned = local[:, part] + fold(dot(mix, xf[:, part]), K)
        for i in range(nodes):
            flat[pl.ds(c * nodes + i, K, stride=M), :] = turned[:, i * cz : (i + 1) * cz]
        copies.append(pltpu.make_async_copy(d_nat.at[:, c], d_hbm.at[:, c], sem.at[2 + c]))
        copies[-1].start()
    for copy in copies:
        copy.wait()


def on_device(axes, sizes, solution, residual, direction, mass, coarse_basis, line_inverse, coarse_factor):
    K, comps, cx, cy, cz = direction.shape
    n = sizes[0] * sizes[1]
    NC = coarse_factor.shape[1]
    nodes, M = cx * cy, comps * cx * cy
    assert K * NC == n * TILE * cz and K <= n and 4 * K <= cz and WIDTH * cy == TILE
    flat = (K, comps, nodes, cz)
    vmem = pl.BlockSpec(memory_space=pltpu.VMEM)
    hbm = pl.BlockSpec(memory_space=pltpu.HBM)
    dma = pltpu.SemaphoreType.DMA
    natural = pltpu.VMEM(flat, F32)
    wide = pltpu.VMEM((K, M * cz), F32)
    across = pltpu.VMEM((comps, K, WIDTH * cy, cz), F32)
    beside = pltpu.VMEM((K, comps * cx * WIDTH * cz), F32)
    slots = pltpu.VMEM((n, SLOT, cz), F32)
    tiles, line = (pltpu.VMEM((count, TILE, cz), F32) for count in (n, sizes[0]))
    inputs = (
        direction.reshape(flat), residual.reshape(flat), solution.reshape(flat), coarse_basis.reshape(flat),
        mass.reshape(nodes, cz), line_inverse.reshape(cz, cz), coarse_factor,
    )
    outs = pl.pallas_call(
        functools.partial(step_kernel, axes, sizes),
        out_shape=[
            jax.ShapeDtypeStruct(flat, F32), jax.ShapeDtypeStruct(flat, F32), jax.ShapeDtypeStruct((K, M * cz), F32),
            jax.ShapeDtypeStruct((4 * K, M * cz), BF16), jax.ShapeDtypeStruct((2 * K, 4 * K), BF16),
        ],
        in_specs=[hbm] * 7,
        out_specs=[vmem] * 5,
        scratch_shapes=[
            natural, natural, natural, natural, wide, wide,
            pltpu.VMEM((4 * K, M * cz), BF16), pltpu.VMEM((2 * K, M * cz), BF16), pltpu.VMEM((2 * K, M * cz), BF16),
            pltpu.VMEM((2 * K, NC), BF16),
            across, across, beside, beside,
            tiles, pltpu.VMEM((sizes[1], sizes[0], TILE, cz), F32), line, line, tiles, tiles, tiles, tiles,
            slots, slots, slots,
            pltpu.VMEM((nodes, cz), F32), pltpu.VMEM((cz, cz), F32), pltpu.VMEM(coarse_factor.shape, F32),
            dma((7,)), dma((4,)), dma((2, comps)), dma((2,)), dma((16,)),
            pltpu.SemaphoreType.REGULAR((2, max(len(reaches(sizes)), 1))),
        ],
        compiler_params=pltpu.CompilerParams(collective_id=0, has_side_effects=True, vmem_limit_bytes=40 << 20),
    )(*[pltpu.with_memory_space_constraint(array, pltpu.HBM) for array in inputs])
    outs = pl.pallas_call(
        write_kernel,
        out_shape=[jax.ShapeDtypeStruct(flat, F32)] * 3,
        in_specs=[vmem] * 5,
        out_specs=[hbm] * 3,
        scratch_shapes=[natural, dma((2 + comps,))],
        compiler_params=pltpu.CompilerParams(vmem_limit_bytes=8 << 20),
    )(*outs)
    return tuple(out.reshape(direction.shape) for out in outs)


def solution(mesh):
    axes = tuple(mesh.axis_names)
    sizes = tuple(mesh.shape[a] for a in axes)
    sub, inner = axes
    field = P(None, None, sub, inner, None)
    return jax.shard_map(
        functools.partial(on_device, axes, sizes),
        mesh=mesh,
        in_specs=(field, field, field, P(sub, inner, None), field, P(sub, inner, None, None), P((sub, inner), None)),
        out_specs=(field, field, field),
        check_vma=False,
    )
```
